256 devices in a mesh: dp: 128 (over x, z, y_hi, core), mp: 2 (over y_lo).
Axes of the slice: x: 4, y: 4 (y_hi: 2, y_lo: 2; y = y_hi * 2 + y_lo), z: 8, core: 2. Of those that a mesh axis runs over, the one named last changes fastest.
Arguments:
- tokens: bfloat16 [20480, 1024], P('dp', 'mp'), may hold values from -6 to 6
- slot_embed: bfloat16 [20480, 1024], P('dp', 'mp'), may hold values from -0.1875 to 0.1875
- price_units: int32 [20480], P('dp'), may hold values from 0 to 1535
- unassigned: int32 [20480], P('dp'), may hold values from 0 to 1, as said below
Outputs:
- new_prices: float32 [20480], P(('dp', 'mp'))
- margins: float32 [20480], P('dp')
- unassigned_count: int32 [], replicated
The draws below stay inside these ranges and needn't reach their ends.
Inputs may be any that keep to these rules, and one draw needn't show every extreme that they name: At most 128 of the 160 tokens of each index of dp are unassigned, and some index of dp has exactly 128 in every draw.
All inputs are finite; a program needn't handle non-finite values.
Results may differ from the reference program's by a relative error of at most 0.0004.
Values may be sent and summed in bfloat16 or wider, within the bound.
A program may use at most 128 MiB of HBM per device.

```python
import jax
import jax.numpy as jnp
from jax import lax

D = 1024
TOK_DEV = 160
BUSY = 128
TOKENS = 20480
SLOTS = 20480


def draw_unassigned(key, part):
    groups = TOKENS // TOK_DEV
    floor_count = max(BUSY // 8, 1)
    group_ids = jnp.arange(groups, dtype=jnp.int32)
    base_count = floor_count + (BUSY - floor_count) * (group_ids + 1) * (group_ids + 1) // (groups * groups)
    jitter = jax.random.randint(jax.random.fold_in(key, 11), (groups,), -(floor_count // 2), floor_count // 2 + 1)
    counts = jnp.clip(base_count + jitter, 1, BUSY)
    hot_group = groups - 1 - jax.random.randint(jax.random.fold_in(key, 12), (), 0, max(groups // 4, 1))
    counts = jnp.where(group_ids == hot_group, BUSY, counts)
    noise_bits = jax.random.randint(jax.random.fold_in(key, 13), (groups, TOK_DEV), 0, 1 << 20)
    sort_keys = noise_bits * TOK_DEV + jnp.arange(TOK_DEV, dtype=jnp.int32)[None, :]
    ordering = jnp.argsort(sort_keys, axis=1)
    ranking = jnp.argsort(ordering, axis=1)
    return (ranking < counts[:, None]).astype(jnp.int32).reshape(TOKENS)


def with_ends(entries, key, smallest, high):
    longest = entries.shape.index(max(entries.shape))
    spots = []
    for shift in (0, 1):
        where = [jax.random.randint(jax.random.fold_in(key, axis), (), 0, length) for axis, length in enumerate(entries.shape)]
        where[longest] = (where[longest] + shift) % entries.shape[longest]
        spots.append(tuple(where))
    return entries.at[spots[0]].set(smallest).at[spots[1]].set(high)


def steps_of(key, dims, cuts, low, high):
    def one(position, shards_of):
        draws = jax.random.uniform(jax.random.fold_in(jax.random.fold_in(key, 6), position), (shards_of,), jnp.float32, low / len(cuts), high / len(cuts))
        return jnp.repeat(jnp.exp(draws), dims[position] // shards_of).reshape((-1,) + (1,) * (len(dims) - position - 1))

    loudness = one(*cuts[0])
    for cut in cuts[1:]:
        loudness = loudness * one(*cut)
    return loudness


def gaussian(key, dims, deviation, bound, cuts=(), kind=jnp.bfloat16):
    values = deviation * jax.random.normal(key, dims, jnp.float32)
    if cuts:
        values = values * steps_of(key, dims, cuts, -0.22, 0.18)
    return jnp.clip(values, -bound, bound).astype(kind)


def setup_inputs(seed: int = 0) -> dict:
    key_list = jax.random.split(jax.random.key(seed), 5)
    tokens = gaussian(key_list[0], (TOKENS, D), 1.0, 6.0, ((0, 128), (1, 2)))
    slot_embed = gaussian(key_list[1], (SLOTS, D), D ** -0.5, 0.1875, ((0, 128), (1, 2)))
    price_units = with_ends(jax.random.randint(key_list[2], (SLOTS,), 0, 1536), jax.random.fold_in(key_list[2], 1), 0, 1535).astype(jnp.int32)
    unassigned = draw_unassigned(jax.random.fold_in(key_list[4], 71), 0)
    return dict(tokens=tokens, slot_embed=slot_embed, price_units=price_units, unassigned=unassigned)


unit_price = 1.0 / 512.0


def top_two(values):
    best_value = jnp.max(values, axis=1)
    where_best = jnp.argmax(values, axis=1).astype(jnp.int32)
    column_ids = lax.broadcasted_iota(jnp.int32, values.shape, 1)
    second_value = jnp.max(jnp.where(column_ids == where_best[:, None], -jnp.inf, values), axis=1)
    return best_value, second_value


def reference(tokens, slot_embed, price_units, unassigned):
    prices = price_units.astype(jnp.float32) * unit_price
    groups = TOKENS // TOK_DEV
    token_blocks = tokens.reshape(groups, TOK_DEV, D)
    mask_blocks = unassigned.reshape(groups, TOK_DEV)

    def advance(highest, inputs):
        token_rows, is_live = inputs
        scores = jnp.dot(token_rows, slot_embed.T, preferred_element_type=jnp.float32)
        values = scores - prices[None, :]
        best_value, second_value = top_two(values)
        margin_rows = jnp.where(is_live > 0, best_value - second_value, jnp.float32(0.0))
        excess = jnp.where(is_live[:, None] > 0, values - second_value[:, None], -jnp.inf)
        return jnp.maximum(highest, jnp.max(excess, axis=0)), margin_rows

    initial = jnp.zeros((SLOTS,), jnp.float32)
    highest, margin_blocks = lax.scan(advance, initial, (token_blocks, mask_blocks))
    new_prices = prices + highest
    margins = margin_blocks.reshape(TOKENS)
    unassigned_count = jnp.sum(unassigned).astype(jnp.int32)
    return (new_prices, margins, unassigned_count)
```

```python
import jax
import jax.numpy as jnp
from jax import lax
from jax.experimental import pallas as pl
from jax.experimental.pallas import tpu as pltpu
from jax.sharding import PartitionSpec as P

MESH = pl.DeviceIdType.MESH
X, Y, Z, C = 4, 4, 8, 2
BUSY = 128
HALF = 80
WIDTH = 512
GROUPS = 8
OWNERS = 16
OFFS = (0, -1, 1, 2)
UNIT = 1.0 / 512.0


def wrap(v, n):
    return lax.rem(v + n, n)


def merge(a1, a2, b1, b2):
    return jnp.maximum(a1, b1), jnp.maximum(jnp.minimum(a1, b1), jnp.maximum(a2, b2))


def kernel(
    tok_hbm, slot_hbm, unit_hbm, mask_hbm, price_out, margin_out, count_out,
    tok, give, units, mask, hot, bid, slt, prow, prep, flg, val, t2, col, rz,
    lsem, xs, xr, bs, br, zs, zr, ss, sr, ps, pr, fs, fr, ts, tr, cs, cr,
):
    dp, yl = lax.axis_index("dp"), lax.axis_index("mp")
    c, yh = lax.rem(dp, 2), lax.rem(dp // 2, 2)
    z, x = lax.rem(dp // 4, Z), dp // 32
    y = yh * 2 + yl
    own = z * 2 + c
    grp = x * 2 + yh

    def dev(x_, y_, z_, c_):
        return (((x_ * Z + z_) * 2 + y_ // 2) * 2 + c_, lax.rem(y_, 2))

    started = []

    def send(src, dst, ssem, rsem, to):
        copy = pltpu.make_async_remote_copy(
            src_ref=src, dst_ref=dst, send_sem=ssem, recv_sem=rsem, device_id=to, device_id_type=MESH
        )
        copy.start()
        started.append(copy)

    def arrived(dst, ssem, rsem):
        pltpu.make_async_remote_copy(
            src_ref=dst, dst_ref=dst, send_sem=ssem, recv_sem=rsem,
            device_id=dev(x, y, z, 1 - c), device_id_type=MESH,
        ).wait_recv()

    plane = [(dx, dy) for dx in range(X) for dy in range(Y) if dx or dy]
    column = [(dz, dc) for dz in range(Z) for dc in range(C) if dz or dc]

    def in_plane(dx, dy):
        return dev(wrap(x + dx, X), wrap(y + dy, Y), z, c)

    def in_column(dz, dc):
        return dev(x, y, wrap(z + dz, Z), wrap(c + dc, C))

    keep = pl.ds(pl.multiple_of(yl * HALF, 16), HALF)
    away = pl.ds(pl.multiple_of((1 - yl) * HALF, 16), HALF)
    loads = [
        pltpu.make_async_copy(mask_hbm, mask, lsem.at[0]),
        pltpu.make_async_copy(slot_hbm.at[away], give, lsem.at[1]),
        pltpu.make_async_copy(slot_hbm.at[keep], slt.at[yl, own], lsem.at[2]),
        pltpu.make_async_copy(tok_hbm, tok, lsem.at[3]),
        pltpu.make_async_copy(unit_hbm, units, lsem.at[4]),
    ]
    for load in loads:
        load.start()
    barrier = pltpu.get_barrier_semaphore()
    for dx, dy in plane:
        pl.semaphore_signal(barrier, inc=1, device_id=in_plane(dx, dy), device_id_type=MESH)
    for dz, dc in column:
        pl.semaphore_signal(barrier, inc=1, device_id=in_column(dz, dc), device_id_type=MESH)

    loads[0].wait()
    live = mask[...]
    length = live.shape[1]
    before = lax.broadcasted_iota(jnp.int32, (length, length), 0) <= lax.broadcasted_iota(
        jnp.int32, (length, length), 1
    )
    live8 = jnp.broadcast_to(live.astype(jnp.float32), (8, length))
    rank = jnp.dot(
        live8.astype(jnp.bfloat16), before.astype(jnp.float32).astype(jnp.bfloat16), preferred_element_type=jnp.float32
    )
    rank = jnp.where(live8 > 0, rank, 0.0)[0:1, :]
    places = lax.broadcasted_iota(jnp.int32, (BUSY, length), 0).astype(jnp.float32) + 1.0
    hot[...] = jnp.where(places == rank, 1.0, 0.0)
    loads[3].wait()
    bid[yl, grp] = jnp.dot(
        hot[...].astype(jnp.bfloat16), tok[...], preferred_element_type=jnp.float32
    ).astype(jnp.bfloat16)
    total = jnp.sum(live.astype(jnp.float32), axis=1, keepdims=True)
    lanes = lax.broadcasted_iota(jnp.int32, (1, BUSY), 1)
    flg[grp] = jnp.where(lanes.astype(jnp.float32) < total, 1.0, 0.0)
    loads[4].wait()
    both = units[...].astype(jnp.float32) * UNIT
    mine = jnp.where(yl == 0, both[:, 0:HALF], both[:, HALF : 2 * HALF])
    prow[own] = jnp.concatenate([mine, jnp.zeros((1, 128 - HALF), jnp.float32)], axis=1)
    loads[1].wait()
    loads[2].wait()
    pl.semaphore_wait(barrier, len(plane) + len(column))

    halves = (yl, 1 - yl)
    reach = ((4, 3), (3, 4))

    def z_send(t, way, k):
        step = 1 if way == 0 else -1
        chunk = slt.at[halves[t], wrap(z - step * k, Z) * 2 + c]
        send(chunk, chunk, zs.at[t, way, k], zr.at[t, way, k], in_column(step, 0))

    def sib_send(t, off):
        chunk = slt.at[halves[t], wrap(z + off, Z) * 2 + c]
        send(chunk, chunk, ss.at[t, off % Z], sr.at[t, off % Z], in_column(0, 1))

    def z_take(t, way, k):
        step = 1 if way == 0 else -1
        off = -step * (k + 1)
        arrived(slt.at[halves[t], wrap(z + off, Z) * 2 + c], zs.at[t, way, k], zr.at[t, way, k])
        if k + 1 < reach[t][way]:
            z_send(t, way, k + 1)
        sib_send(t, off)

    def piece(dx, dy, part, lo=0, hi=64):
        ya = wrap(y + dy, Y)
        return bid.at[lax.rem(ya, 2), wrap(x + dx, X) * 2 + ya // 2, pl.ds(part * 64 + lo, hi - lo)]

    def ring(part, j):
        along_x = (part == 0) == (j == 0)
        base = (0, 0) if j == 0 else ((OFFS[j - 1], 0) if part == 0 else (0, OFFS[j - 1]))

        def at(k, lo=0, hi=64):
            return piece(base[0] + (k if along_x else 0), base[1] + (0 if along_x else k), part, lo, hi)

        def to(k):
            return in_plane(k, 0) if along_x else in_plane(0, k)

        return at, to

    def b_send(part, j):
        at, to = ring(part, j)
        for kind, k in ((0, 1), (1, -1)):
            send(at(0), at(0), bs.at[part, j, kind], br.at[part, j, kind], to(k))

    def b_take(part, j, kind):
        at, to = ring(part, j)
        k = 1 if kind == 0 else -1
        arrived(at(-k), bs.at[part, j, kind], br.at[part, j, kind])
        lo = 0 if kind == 0 else 32
        half = at(-k, lo, lo + 32)
        send(half, half, bs.at[part, j, kind + 2], br.at[part, j, kind + 2], to(k))

    def b_far(part, j):
        at, _ = ring(part, j)
        arrived(at(2, 0, 32), bs.at[part, j, 2], br.at[part, j, 2])
        arrived(at(2, 32, 64), bs.at[part, j, 3], br.at[part, j, 3])

    send(give, slt.at[yl, own], xs, xr, dev(x, yh * 2 + 1 - yl, z, c))
    z_send(0, 0, 0)
    z_send(0, 1, 0)
    sib_send(0, 0)
    for part in (0, 1):
        b_send(part, 0)
    for dx in range(X):
        for dh in range(2):
            if dx or dh:
                send(flg.at[grp], flg.at[grp], fs.at[dx, dh], fr.at[dx, dh], in_plane(dx, 2 * dh))
    for dz, dc in column:
        send(prow.at[own], prow.at[own], ps.at[dz, dc], pr.at[dz, dc], in_column(dz, dc))
    for part in (0, 1):
        b_send(part, 1)
    for part in (0, 1):
        for kind in (0, 1):
            b_take(part, 0, kind)
            b_send(part, 2 + kind)
    arrived(slt.at[1 - yl, own], xs, xr)
    z_send(1, 0, 0)
    z_send(1, 1, 0)
    sib_send(1, 0)
    z_take(0, 0, 0)
    z_take(0, 1, 0)
    for part in (0, 1):
        for kind in (0, 1):
            b_take(part, 1, kind)
    for part in (0, 1):
        b_far(part, 0)
        b_send(part, 4)
    z_take(1, 0, 0)
    z_take(1, 1, 0)
    z_take(0, 0, 1)
    z_take(0, 1, 1)
    for j in (2, 3):
        for part in (0, 1):
            for kind in (0, 1):
                b_take(part, j, kind)
    z_take(1, 0, 1)
    z_take(1, 1, 1)
    z_take(0, 0, 2)
    z_take(0, 1, 2)
    for part in (0, 1):
        for kind in (0, 1):
            b_take(part, 4, kind)
    z_take(1, 0, 2)
    z_take(1, 1, 2)
    z_take(0, 0, 3)
    z_take(1, 1, 3)
    for dz, dc in column:
        arrived(prow.at[wrap(z - dz, Z) * 2 + wrap(c - dc, C)], ps.at[dz, dc], pr.at[dz, dc])
    for s in range(OWNERS):
        prep[s] = jnp.broadcast_to(prow[s], (128, 128)).T[0:HALF, :]
    for part in (0, 1):
        for j in (1, 2, 3, 4):
            b_far(part, j)
    for t in (0, 1):
        for off in range(Z):
            arrived(slt.at[halves[t], wrap(z + off, Z) * 2 + 1 - c], ss.at[t, off], sr.at[t, off])

    low = jnp.full((8, 256), -jnp.inf, jnp.float32)
    firsts, seconds = [], []
    tile = 4
    for n in range(4):
        m1, m2 = low, low

        def step(i, carry, n=n):
            m1, m2 = carry
            acc = jnp.zeros((tile * HALF, 256), jnp.float32)
            for h in range(2):
                acc += lax.dot_general(
                    slt[h, pl.ds(i * tile, tile)].reshape(tile * HALF, WIDTH),
                    bid[h, 2 * n : 2 * n + 2].reshape(256, WIDTH),
                    (((1,), (1,)), ((), ())),
                    preferred_element_type=jnp.float32,
                )
            price = prep[pl.ds(i * tile, tile)].reshape(tile * HALF, 128)
            v = acc - jnp.concatenate([price, price], axis=1)
            val[n, pl.ds(i * tile, tile)] = v.reshape(tile, HALF, 256)
            for r in range(tile * HALF // 8):
                row = v[r * 8 : r * 8 + 8, :]
                m2 = jnp.maximum(m2, jnp.minimum(m1, row))
                m1 = jnp.maximum(m1, row)
            return m1, m2

        m1, m2 = lax.fori_loop(0, OWNERS // tile, step, (m1, m2))
        for shift in (4, 2, 1):
            m1, m2 = merge(m1, m2, pltpu.roll(m1, shift, 0), pltpu.roll(m2, shift, 0))
        firsts += [m1[:, 0:128], m1[:, 128:256]]
        seconds += [m2[:, 0:128], m2[:, 128:256]]
    sub = lax.broadcasted_iota(jnp.int32, (8, 128), 0)
    f, s2 = firsts[0], seconds[0]
    for g in range(1, GROUPS):
        f = jnp.where(sub == g, firsts[g], f)
        s2 = jnp.where(sub == g, seconds[g], s2)
    q = x * 4 + y
    t2[q, 0] = f
    t2[q, 1] = s2
    for dx, dy in plane:
        send(t2.at[q], t2.at[q], ts.at[dx, dy], tr.at[dx, dy], in_plane(dx, dy))
    for dx in range(X):
        for dh in range(2):
            if dx or dh:
                src = wrap(x - dx, X) * 2 + wrap(yh - dh, 2)
                arrived(flg.at[src], fs.at[dx, dh], fr.at[dx, dh])
    bidders = flg[0]
    for g in range(1, GROUPS):
        bidders = bidders + flg[g]
    bidders = jnp.sum(bidders, axis=1, keepdims=True)
    for dx, dy in plane:
        src = wrap(x - dx, X) * 4 + wrap(y - dy, Y)
        arrived(t2.at[src], ts.at[dx, dy], tr.at[dx, dy])
    for i in range(16):
        if i == 0:
            f, s2 = t2[0, 0], t2[0, 1]
        else:
            f, s2 = merge(f, s2, t2[i, 0], t2[i, 1])

    bars = [
        jnp.broadcast_to(jnp.where(flg[g] > 0, s2[g : g + 1, :], jnp.inf), (HALF, 128)) for g in range(GROUPS)
    ]
    for s in range(OWNERS):
        top = jnp.full((HALF, 128), -jnp.inf, jnp.float32)
        for g in range(GROUPS):
            top = jnp.maximum(top, val[g // 2, s, :, (g % 2) * 128 : (g % 2) * 128 + 128] - bars[g])
        row = jnp.max(top.T, axis=0, keepdims=True)
        row = jnp.concatenate([row, jnp.zeros((1, 128 - HALF), jnp.float32)], axis=1)
        col[s] = jnp.where(lanes == 127, bidders, row)
    rz[own] = col[own]
    for dz, dc in column:
        send(
            col.at[wrap(z + dz, Z) * 2 + wrap(c + dc, C)], rz.at[own], cs.at[dz, dc], cr.at[dz, dc], in_column(dz, dc)
        )
    gap = jnp.where(flg[grp] > 0, jnp.max(jnp.where(sub == grp, f - s2, -jnp.inf), axis=0, keepdims=True), 0.0)
    margin_out[...] = jnp.dot(
        jnp.broadcast_to(gap, (8, 128)), hot[...], precision=lax.Precision.HIGHEST, preferred_element_type=jnp.float32
    )[0:1, :]
    for dz, dc in column:
        arrived(rz.at[wrap(z - dz, Z) * 2 + wrap(c - dc, C)], cs.at[dz, dc], cr.at[dz, dc])
    best, count = rz[0], rz[0]
    for s in range(1, OWNERS):
        best = jnp.maximum(best, rz[s])
        count = count + rz[s]
    price_out[...] = (prow[own] + jnp.maximum(best, 0.0))[:, 0:HALF]
    count_out[...] = count[:, 127:128].astype(jnp.int32)
    for copy in started:
        copy.wait_send()


def on_device(tokens, slot_embed, price_units, unassigned):
    length = unassigned.shape[0]
    dma, anyspace = pltpu.SemaphoreType.DMA, pl.BlockSpec(memory_space=pl.ANY)
    vmem = pl.BlockSpec(memory_space=pltpu.VMEM)
    f32, bf16 = jnp.float32, jnp.bfloat16
    new_prices, margins, count = pl.pallas_call(
        kernel,
        out_shape=(
            jax.ShapeDtypeStruct((1, HALF), f32),
            jax.ShapeDtypeStruct((1, length), f32),
            jax.ShapeDtypeStruct((1, 1), jnp.int32),
        ),
        in_specs=[anyspace] * 4,
        out_specs=(vmem, vmem, vmem),
        scratch_shapes=[
            pltpu.VMEM((length, WIDTH), bf16),
            pltpu.VMEM((HALF, WIDTH), bf16),
            pltpu.VMEM((1, length), jnp.int32),
            pltpu.VMEM((1, length), jnp.int32),
            pltpu.VMEM((BUSY, length), f32),
            pltpu.VMEM((2, GROUPS, BUSY, WIDTH), bf16),
            pltpu.VMEM((2, OWNERS, HALF, WIDTH), bf16),
            pltpu.VMEM((OWNERS, 1, 128), f32),
            pltpu.VMEM((OWNERS, HALF, 128), f32),
            pltpu.VMEM((GROUPS, 1, 128), f32),
            pltpu.VMEM((4, OWNERS, HALF, 256), f32),
            pltpu.VMEM((16, 2, 8, 128), f32),
            pltpu.VMEM((OWNERS, 1, 128), f32),
            pltpu.VMEM((OWNERS, 1, 128), f32),
            dma((5,)),
            dma, dma,
            dma((2, 5, 4)), dma((2, 5, 4)),
            dma((2, 2, 4)), dma((2, 2, 4)),
            dma((2, Z)), dma((2, Z)),
            dma((Z, C)), dma((Z, C)),
            dma((X, 2)), dma((X, 2)),
            dma((X, Y)), dma((X, Y)),
            dma((Z, C)), dma((Z, C)),
        ],
        compiler_params=pltpu.CompilerParams(collective_id=0, has_side_effects=True, vmem_limit_bytes=32 << 20),
    )(tokens, slot_embed, price_units.reshape(1, length), unassigned.reshape(1, length))
    return new_prices.reshape(HALF), margins.reshape(length), count.reshape(())


def solution(mesh):
    return jax.shard_map(
        on_device,
        mesh=mesh,
        in_specs=(P("dp", "mp"), P("dp", "mp"), P("dp"), P("dp")),
        out_specs=(P(("dp", "mp")), P("dp"), P()),
        check_vma=False,
    )
```

```python
import jax
import jax.numpy as jnp
from jax import lax
from jax.experimental import pallas as pl
from jax.experimental.pallas import tpu as pltpu
from jax.sharding import PartitionSpec as P

MESH = pl.DeviceIdType.MESH
X, Y, Z, C = 4, 4, 8, 2
BUSY = 128
HALF = 80
WIDTH = 512
GROUPS = 8
OWNERS = 16
OFFS = (0, -1, 1, 2)
UNIT = 1.0 / 512.0
PLAN = (
    (1, 2, 0), (1, 2, 1), (1, 2, 2), (1, 1, 0, 0, 0, 0), (1, 1, 0, 0, 1, 0), (1, 1, 0, 1, 1, 0), (1, 1, 0, 2, 0, 0),
    (1, 1, 0, 3, 1, 0), (1, 1, 0, 4, 0, 0), (1, 2, 3), (1, 1, 0, 1, 0, 0), (1, 1, 0, 2, 1, 0), (1, 2, 4),
    (1, 1, 0, 3, 0, 0), (1, 1, 0, 4, 1, 0), (2,), (1, 0, 0, 0, 0, 0), (1, 0, 0, 0, 0, 1), (1, 0, 1, 0, 0, 0),
    (1, 0, 1, 0, 0, 1), (1, 0, 0, 0, 1, 1), (1, 0, 0, 0, 1, 0), (1, 0, 1, 0, 1, 1), (1, 0, 1, 0, 1, 0),
    (1, 0, 0, 1, 0, 0), (1, 0, 1, 1, 0, 0), (1, 0, 1, 1, 0, 1), (1, 0, 0, 1, 1, 1), (1, 0, 1, 1, 1, 1),
    (1, 0, 1, 1, 1, 0), (0, 2, 0), (1, 1, 1, 0, 0, 0), (1, 1, 1, 0, 1, 0), (0, 1, 0, 0, 0, 0), (0, 1, 0, 0, 1, 0),
    (1, 1, 0, 0, 0, 1), (1, 1, 0, 0, 1, 1), (0, 2, 1), (1, 1, 1, 1, 0, 0), (1, 1, 1, 1, 1, 0), (0, 1, 0, 1, 1, 0),
    (0, 1, 0, 2, 0, 0), (1, 1, 0, 1, 1, 1), (1, 1, 0, 2, 0, 1), (1, 0, 0, 1, 0, 1), (1, 0, 0, 1, 1, 0), (0, 2, 2),
    (1, 1, 1, 2, 0, 0), (1, 1, 1, 2, 1, 0), (0, 1, 0, 3, 1, 0), (0, 1, 0, 4, 0, 0), (1, 1, 0, 3, 1, 1),
    (1, 1, 0, 4, 0, 1), (0, 0, 0, 0, 0, 0), (0, 0, 0, 0, 0, 1), (1, 0, 0, 0, 0, 2), (1, 0, 0, 2, 0, 0),
    (1, 0, 0, 3, 0, 0), (0, 2, 3), (1, 1, 1, 3, 0, 0), (1, 1, 1, 3, 1, 0), (0, 1, 0, 1, 0, 0), (0, 1, 0, 2, 1, 0),
    (1, 1, 0, 1, 0, 1), (1, 1, 0, 2, 1, 1), (0, 2, 4), (1, 1, 1, 4, 0, 0), (1, 1, 1, 4, 1, 0), (0, 1, 0, 3, 0, 0),
    (0, 1, 0, 4, 1, 0), (1, 1, 0, 3, 0, 1), (0, 0, 1, 0, 0, 0), (1, 0, 1, 0, 0, 2), (1, 0, 1, 2, 0, 0),
    (1, 0, 1, 2, 0, 1), (0, 0, 0, 0, 1, 0), (0, 0, 0, 0, 1, 1), (1, 0, 0, 2, 1, 1), (1, 0, 0, 0, 1, 2),
    (1, 0, 0, 3, 1, 1), (1, 1, 0, 4, 1, 1), (0, 0, 1, 0, 0, 1), (0, 0, 1, 0, 1, 1), (1, 0, 1, 3, 0, 0),
    (1, 0, 1, 3, 0, 1), (1, 0, 1, 0, 1, 2), (1, 0, 1, 3, 1, 1), (1, 0, 1, 3, 1, 0), (1, 0, 0, 2, 0, 1),
    (0, 0, 1, 0, 1, 0), (1, 0, 1, 2, 1, 1), (1, 0, 1, 2, 1, 0), (0, 1, 1, 0, 0, 0), (0, 1, 1, 0, 1, 0),
    (1, 1, 1, 0, 1, 1), (1, 1, 1, 0, 0, 1), (0, 0, 1, 1, 0, 0), (0, 0, 1, 1, 1, 1), (0, 1, 0, 0, 0, 1),
    (0, 1, 0, 0, 1, 1), (1, 1, 0, 0, 0, 2), (1, 0, 1, 1, 0, 2), (0, 1, 1, 1, 0, 0), (1, 1, 1, 1, 0, 1),
    (1, 0, 0, 2, 1, 0), (1, 0, 1, 1, 1, 2), (0, 0, 0, 1, 1, 1), (0, 0, 1, 1, 0, 1), (0, 0, 1, 1, 1, 0),
    (0, 1, 1, 1, 1, 0), (1, 1, 1, 1, 1, 1), (1, 0, 0, 3, 0, 1), (0, 0, 0, 1, 0, 0), (0, 1, 1, 2, 1, 0),
    (1, 1, 1, 2, 1, 1), (0, 1, 0, 1, 1, 1), (1, 1, 0, 1, 1, 2), (0, 1, 0, 2, 0, 1), (1, 1, 0, 2, 0, 2),
    (1, 0, 0, 3, 1, 0), (0, 1, 1, 3, 0, 0), (1, 1, 1, 3, 0, 1), (0, 1, 1, 4, 1, 0), (1, 1, 1, 4, 1, 1),
    (0, 1, 1, 2, 0, 0), (1, 1, 1, 2, 0, 1), (0, 0, 0, 0, 0, 2), (1, 0, 0, 4, 0, 0), (1, 0, 0, 4, 0, 1),
    (0, 1, 0, 4, 0, 1), (1, 1, 0, 4, 0, 2), (0, 1, 0, 3, 1, 1), (1, 1, 0, 3, 1, 2), (0, 1, 1, 3, 1, 0),
    (1, 1, 1, 3, 1, 1), (0, 0, 0, 2, 0, 0), (0, 0, 1, 0, 0, 2), (1, 0, 1, 4, 0, 0), (1, 0, 1, 4, 0, 1),
    (0, 1, 1, 4, 0, 0), (1, 1, 1, 4, 0, 1), (0, 0, 0, 0, 1, 2), (1, 0, 0, 4, 1, 1), (1, 0, 0, 4, 1, 0),
    (0, 0, 1, 2, 0, 0), (1, 0, 0, 1, 1, 2), (0, 0, 0, 2, 1, 1), (0, 0, 0, 3, 0, 0), (0, 0, 1, 0, 1, 2),
    (1, 0, 1, 4, 1, 1), (1, 0, 1, 4, 1, 0), (1, 1, 0, 0, 1, 2), (0, 0, 0, 1, 0, 1), (0, 0, 0, 1, 1, 0),
    (0, 1, 1, 0, 1, 1), (1, 1, 1, 0, 1, 2), (0, 1, 0, 1, 0, 1), (1, 0, 0, 1, 0, 2), (1, 1, 0, 1, 0, 2),
    (0, 0, 1, 3, 0, 0), (0, 1, 0, 2, 1, 1), (0, 1, 1, 1, 0, 1), (1, 1, 1, 1, 0, 2), (1, 0, 1, 3, 0, 2),
    (1, 1, 0, 2, 1, 2), (0, 0, 1, 2, 0, 1), (0, 0, 0, 3, 1, 1), (1, 0, 1, 2, 0, 2), (0, 0, 1, 2, 1, 1),
    (0, 0, 1, 3, 1, 1), (1, 0, 1, 2, 1, 2), (1, 0, 1, 3, 1, 2), (0, 1, 0, 3, 0, 1), (1, 1, 0, 3, 0, 2),
    (0, 1, 1, 2, 1, 1), (1, 1, 1, 2, 1, 2), (0, 0, 1, 3, 0, 1), (0, 1, 0, 4, 1, 1), (1, 1, 0, 4, 1, 2),
    (1, 0, 0, 2, 1, 2), (0, 1, 1, 3, 0, 1), (1, 1, 1, 3, 0, 2), (1, 0, 0, 2, 0, 2), (0, 0, 1, 3, 1, 0),
    (0, 1, 1, 4, 1, 1), (1, 1, 1, 4, 1, 2), (1, 0, 0, 3, 1, 2), (0, 1, 1, 0, 0, 1), (1, 1, 1, 0, 0, 2),
    (0, 1, 0, 0, 0, 2), (1, 1, 0, 0, 0, 3), (1, 0, 0, 3, 0, 2), (0, 0, 0, 2, 0, 1), (0, 0, 1, 2, 1, 0),
    (0, 1, 1, 1, 1, 1), (1, 1, 1, 1, 1, 2), (0, 0, 0, 4, 0, 0), (1, 0, 0, 4, 0, 2), (0, 1, 0, 1, 1, 2),
    (1, 1, 0, 1, 1, 3), (0, 1, 0, 2, 0, 2), (1, 1, 0, 2, 0, 3), (0, 0, 0, 4, 0, 1), (0, 0, 1, 1, 0, 2),
    (0, 0, 0, 2, 1, 0), (0, 1, 0, 3, 1, 2), (1, 1, 0, 3, 1, 3), (0, 0, 0, 4, 1, 1), (1, 0, 0, 4, 1, 2),
    (0, 1, 1, 2, 0, 1), (1, 1, 1, 2, 0, 2), (0, 0, 1, 1, 1, 2), (0, 1, 0, 4, 0, 2), (1, 1, 0, 4, 0, 3),
    (0, 0, 1, 4, 0, 0), (1, 0, 1, 4, 0, 2), (0, 0, 0, 3, 0, 1), (0, 1, 1, 3, 1, 1), (1, 1, 1, 3, 1, 2),
    (0, 0, 0, 4, 1, 0), (0, 0, 1, 4, 0, 1), (0, 0, 0, 3, 1, 0), (0, 0, 1, 4, 1, 1), (1, 0, 1, 4, 1, 2),
    (0, 1, 1, 0, 1, 2), (0, 1, 1, 4, 0, 1), (1, 1, 1, 0, 1, 3), (1, 1, 1, 4, 0, 2), (0, 0, 1, 4, 1, 0),
    (0, 1, 1, 1, 0, 2), (0, 1, 1, 2, 1, 2), (1, 1, 1, 1, 0, 3), (1, 1, 1, 2, 1, 3), (0, 1, 1, 3, 0, 2),
    (1, 1, 1, 3, 0, 3), (0, 1, 1, 4, 1, 2), (1, 1, 1, 4, 1, 3), (0, 1, 0, 0, 1, 2), (0, 1, 0, 1, 0, 2),
    (0, 0, 0, 1, 1, 2), (0, 1, 0, 2, 1, 2), (0, 1, 0, 3, 0, 2), (0, 0, 0, 1, 0, 2), (0, 0, 1, 2, 1, 2),
    (0, 0, 0, 4, 0, 2), (0, 1, 0, 4, 1, 2), (0, 0, 1, 3, 0, 2), (0, 0, 1, 3, 1, 2), (0, 1, 1, 0, 0, 2),
    (0, 1, 0, 0, 0, 3), (0, 0, 1, 2, 0, 2), (0, 1, 1, 1, 1, 2), (0, 1, 0, 1, 1, 3), (0, 0, 0, 4, 1, 2),
    (0, 0, 1, 4, 0, 2), (0, 0, 0, 2, 1, 2), (0, 1, 0, 2, 0, 3), (0, 0, 0, 2, 0, 2), (0, 0, 1, 4, 1, 2),
    (0, 1, 0, 3, 1, 3), (0, 0, 0, 3, 1, 2), (0, 1, 1, 2, 0, 2), (0, 1, 0, 4, 0, 3), (0, 0, 0, 3, 0, 2),
    (0, 1, 1, 3, 1, 2), (0, 1, 1, 0, 1, 3), (0, 1, 1, 4, 0, 2), (0, 1, 1, 1, 0, 3), (0, 1, 1, 2, 1, 3),
    (0, 1, 1, 3, 0, 3), (0, 1, 1, 4, 1, 3),
)


def wrap(v, n):
    return lax.rem(v + n, n)


def merge(a1, a2, b1, b2):
    return jnp.maximum(a1, b1), jnp.maximum(jnp.minimum(a1, b1), jnp.maximum(a2, b2))


def kernel(
    tok_hbm, slot_hbm, unit_hbm, mask_hbm, price_out, margin_out, count_out,
    tok, give, units, mask, hot, bid, slt, prow, prep, flg, val, t2, col, rz,
    lsem, xs, xr, bs, br, zs, zr, ss, sr, ps, pr, fs, fr, ts, tr, cs, cr,
):
    dp, yl = lax.axis_index("dp"), lax.axis_index("mp")
    c, yh = lax.rem(dp, 2), lax.rem(dp // 2, 2)
    z, x = lax.rem(dp // 4, Z), dp // 32
    y = yh * 2 + yl
    own = z * 2 + c
    grp = x * 2 + yh

    def dev(x_, y_, z_, c_):
        return (((x_ * Z + z_) * 2 + y_ // 2) * 2 + c_, lax.rem(y_, 2))

    started = []

    def send(src, dst, ssem, rsem, to):
        copy = pltpu.make_async_remote_copy(
            src_ref=src, dst_ref=dst, send_sem=ssem, recv_sem=rsem, device_id=to, device_id_type=MESH
        )
        copy.start()
        started.append(copy)

    def arrived(dst, ssem, rsem):
        pltpu.make_async_remote_copy(
            src_ref=dst, dst_ref=dst, send_sem=ssem, recv_sem=rsem,
            device_id=dev(x, y, z, 1 - c), device_id_type=MESH,
        ).wait_recv()

    plane = [(dx, dy) for dx in range(X) for dy in range(Y) if dx or dy]
    column = [(dz, dc) for dz in range(Z) for dc in range(C) if dz or dc]

    def in_plane(dx, dy):
        return dev(wrap(x + dx, X), wrap(y + dy, Y), z, c)

    def in_column(dz, dc):
        return dev(x, y, wrap(z + dz, Z), wrap(c + dc, C))

    keep = pl.ds(pl.multiple_of(yl * HALF, 16), HALF)
    away = pl.ds(pl.multiple_of((1 - yl) * HALF, 16), HALF)
    loads = [
        pltpu.make_async_copy(mask_hbm, mask, lsem.at[0]),
        pltpu.make_async_copy(slot_hbm.at[away], give, lsem.at[1]),
        pltpu.make_async_copy(slot_hbm.at[keep], slt.at[yl, own], lsem.at[2]),
        pltpu.make_async_copy(tok_hbm, tok, lsem.at[3]),
        pltpu.make_async_copy(unit_hbm, units, lsem.at[4]),
    ]
    for load in loads:
        load.start()
    barrier = pltpu.get_barrier_semaphore()
    near = [in_plane(1, 0), in_plane(-1, 0), in_plane(0, 1), in_plane(0, -1)]
    near += [in_column(1, 0), in_column(-1, 0), in_column(0, 1)]
    for to in near:
        pl.semaphore_signal(barrier, inc=1, device_id=to, device_id_type=MESH)
    lanes = lax.broadcasted_iota(jnp.int32, (1, BUSY), 1)
    length = mask.shape[1]

    loads[4].wait()
    both = units[...].astype(jnp.float32) * UNIT
    mine = jnp.where(yl == 0, both[:, 0:HALF], both[:, HALF : 2 * HALF])
    prow[own] = jnp.concatenate([mine, jnp.zeros((1, 128 - HALF), jnp.float32)], axis=1)

    def compact():
        loads[0].wait()
        live = mask[...]
        before = lax.broadcasted_iota(jnp.int32, (length, length), 0) <= lax.broadcasted_iota(
            jnp.int32, (length, length), 1
        )
        live8 = jnp.broadcast_to(live.astype(jnp.float32), (8, length))
        rank = jnp.dot(
            live8.astype(jnp.bfloat16),
            before.astype(jnp.float32).astype(jnp.bfloat16),
            preferred_element_type=jnp.float32,
        )
        rank = jnp.where(live8 > 0, rank, 0.0)[0:1, :]
        places = lax.broadcasted_iota(jnp.int32, (BUSY, length), 0).astype(jnp.float32) + 1.0
        hot[...] = jnp.where(places == rank, 1.0, 0.0)
        total = jnp.sum(live.astype(jnp.float32), axis=1, keepdims=True)
        flg[grp] = jnp.where(lanes.astype(jnp.float32) < total, 1.0, 0.0)
        loads[3].wait()
        bid[yl, grp] = jnp.dot(
            hot[...].astype(jnp.bfloat16), tok[...], preferred_element_type=jnp.float32
        ).astype(jnp.bfloat16)

    loads[1].wait()
    loads[2].wait()
    pl.semaphore_wait(barrier, len(near))

    halves = (yl, 1 - yl)

    def rows_of(t, off, core, p=None):
        chunk = (halves[t], wrap(z + off, Z) * 2 + core)
        return slt.at[chunk] if p is None else slt.at[chunk + (pl.ds(p * 16, 16),)]

    def piece(dx, dy, part, p):
        ya = wrap(y + dy, Y)
        return bid.at[lax.rem(ya, 2), wrap(x + dx, X) * 2 + ya // 2, pl.ds(part * 64 + p * 32, 32)]

    def b_at(part, j, p, k):
        along_x = (part == 0) == (j == 0)
        off = 0 if j == 0 else OFFS[j - 1]
        dx, dy = (off, 0) if part == 0 else (0, off)
        return piece(dx + (k if along_x else 0), dy + (0 if along_x else k), part, p), along_x

    def b_send(part, j, p, kind):
        k = (1, -1, 1 if p == 0 else -1)[kind]
        ref, along_x = b_at(part, j, p, -k if kind == 2 else 0)
        to = in_plane(k, 0) if along_x else in_plane(0, k)
        send(ref, ref, bs.at[part, j, p, kind], br.at[part, j, p, kind], to)

    def b_take(part, j, p, kind):
        arrived(b_at(part, j, p, (-1, 1, 2)[kind])[0], bs.at[part, j, p, kind], br.at[part, j, p, kind])

    def sibling(t, off):
        send(rows_of(t, off, c), rows_of(t, off, c), ss.at[t, off % Z], sr.at[t, off % Z], in_column(0, 1))
        if t == 0:
            row = prow.at[wrap(z + off, Z) * 2 + c]
            send(row, row, ss.at[2, off % Z], sr.at[2, off % Z], in_column(0, 1))

    left = {(t, off): 5 for t in (0, 1) for off in range(Z)}

    def landed(t, off):
        left[t, off % Z] -= 1
        if left[t, off % Z] == 0:
            sibling(t, off)

    def z_send(t, p, way, k):
        step = 1 if way == 0 else -1
        ref = rows_of(t, -step * k, c, p)
        send(ref, ref, zs.at[t, p, way, k], zr.at[t, p, way, k], in_column(step, 0))
        if (t, p) == (0, 0):
            row = prow.at[wrap(z - step * k, Z) * 2 + c]
            send(row, row, ps.at[way, k], pr.at[way, k], in_column(step, 0))

    def z_take(t, p, way, k):
        off = -(k + 1) if way == 0 else k + 1
        arrived(rows_of(t, off, c, p), zs.at[t, p, way, k], zr.at[t, p, way, k])
        if (t, p) == (0, 0):
            arrived(prow.at[wrap(z + off, Z) * 2 + c], ps.at[way, k], pr.at[way, k])
        landed(t, off)

    def x_send(p):
        src = give.at[pl.ds(p * 16, 16)]
        send(src, slt.at[yl, own, pl.ds(p * 16, 16)], xs.at[p], xr.at[p], dev(x, yh * 2 + 1 - yl, z, c))

    def x_take(p):
        arrived(rows_of(1, 0, c, p), xs.at[p], xr.at[p])
        landed(1, 0)

    takes, sends = (b_take, z_take, x_take), (b_send, z_send, x_send)
    for op in PLAN:
        if op[0] == 2:
            sibling(0, 0)
            compact()
        else:
            (takes, sends)[op[0]][op[1]](*op[2:])
    for t in (0, 1):
        for off in range(Z):
            arrived(rows_of(t, off, 1 - c), ss.at[t, off], sr.at[t, off])
            if t == 0:
                arrived(prow.at[wrap(z + off, Z) * 2 + 1 - c], ss.at[2, off], sr.at[2, off])
    for s in range(OWNERS):
        prep[s] = jnp.broadcast_to(prow[s], (128, 128)).T[0:HALF, :]

    low = jnp.full((8, 256), -jnp.inf, jnp.float32)
    firsts, seconds = [], []
    tile = 4
    for n in range(4):
        m1, m2 = low, low

        def step(i, carry, n=n):
            m1, m2 = carry
            acc = jnp.zeros((tile * HALF, 256), jnp.float32)
            for h in range(2):
                acc += lax.dot_general(
                    slt[h, pl.ds(i * tile, tile)].reshape(tile * HALF, WIDTH),
                    bid[h, 2 * n : 2 * n + 2].reshape(256, WIDTH),
                    (((1,), (1,)), ((), ())),
                    preferred_element_type=jnp.float32,
                )
            price = prep[pl.ds(i * tile, tile)].reshape(tile * HALF, 128)
            v = acc - jnp.concatenate([price, price], axis=1)
            val[n, pl.ds(i * tile, tile)] = v.reshape(tile, HALF, 256)
            for r in range(tile * HALF // 8):
                row = v[r * 8 : r * 8 + 8, :]
                m2 = jnp.maximum(m2, jnp.minimum(m1, row))
                m1 = jnp.maximum(m1, row)
            return m1, m2

        m1, m2 = lax.fori_loop(0, OWNERS // tile, step, (m1, m2))
        for shift in (4, 2, 1):
            m1, m2 = merge(m1, m2, pltpu.roll(m1, shift, 0), pltpu.roll(m2, shift, 0))
        firsts += [m1[:, 0:128], m1[:, 128:256]]
        seconds += [m2[:, 0:128], m2[:, 128:256]]
    sub = lax.broadcasted_iota(jnp.int32, (8, 128), 0)
    f, s2 = firsts[0], seconds[0]
    for g in range(1, GROUPS):
        f = jnp.where(sub == g, firsts[g], f)
        s2 = jnp.where(sub == g, seconds[g], s2)
    q = x * 4 + y
    t2[q, 0] = f
    t2[q, 1] = s2
    for dx, dy in plane:
        send(t2.at[q], t2.at[q], ts.at[dx, dy], tr.at[dx, dy], in_plane(dx, dy))
    for dx in range(X):
        for dh in range(2):
            if dx or dh:
                send(flg.at[grp], flg.at[grp], fs.at[dx, dh], fr.at[dx, dh], in_plane(dx, 2 * dh))
    for dx in range(X):
        for dh in range(2):
            if dx or dh:
                src = wrap(x - dx, X) * 2 + wrap(yh - dh, 2)
                arrived(flg.at[src], fs.at[dx, dh], fr.at[dx, dh])
    bidders = flg[0]
    for g in range(1, GROUPS):
        bidders = bidders + flg[g]
    bidders = jnp.sum(bidders, axis=1, keepdims=True)
    for dx, dy in plane:
        src = wrap(x - dx, X) * 4 + wrap(y - dy, Y)
        arrived(t2.at[src], ts.at[dx, dy], tr.at[dx, dy])
    for i in range(16):
        if i == 0:
            f, s2 = t2[0, 0], t2[0, 1]
        else:
            f, s2 = merge(f, s2, t2[i, 0], t2[i, 1])

    bars = [
        jnp.broadcast_to(jnp.where(flg[g] > 0, s2[g : g + 1, :], jnp.inf), (HALF, 128)) for g in range(GROUPS)
    ]
    for s in range(OWNERS):
        top = jnp.full((HALF, 128), -jnp.inf, jnp.float32)
        for g in range(GROUPS):
            top = jnp.maximum(top, val[g // 2, s, :, (g % 2) * 128 : (g % 2) * 128 + 128] - bars[g])
        row = jnp.max(top.T, axis=0, keepdims=True)
        row = jnp.concatenate([row, jnp.zeros((1, 128 - HALF), jnp.float32)], axis=1)
        col[s] = jnp.where(lanes == 127, bidders, row)
    rz[own] = col[own]
    for dz, dc in column:
        send(
            col.at[wrap(z + dz, Z) * 2 + wrap(c + dc, C)], rz.at[own], cs.at[dz, dc], cr.at[dz, dc], in_column(dz, dc)
        )
    gap = jnp.where(flg[grp] > 0, jnp.max(jnp.where(sub == grp, f - s2, -jnp.inf), axis=0, keepdims=True), 0.0)
    margin_out[...] = jnp.dot(
        jnp.broadcast_to(gap, (8, 128)), hot[...], precision=lax.Precision.HIGHEST, preferred_element_type=jnp.float32
    )[0:1, :]
    for dz, dc in column:
        arrived(rz.at[wrap(z - dz, Z) * 2 + wrap(c - dc, C)], cs.at[dz, dc], cr.at[dz, dc])
    best, count = rz[0], rz[0]
    for s in range(1, OWNERS):
        best = jnp.maximum(best, rz[s])
        count = count + rz[s]
    price_out[...] = (prow[own] + jnp.maximum(best, 0.0))[:, 0:HALF]
    count_out[...] = count[:, 127:128].astype(jnp.int32)
    for copy in started:
        copy.wait_send()


def on_device(tokens, slot_embed, price_units, unassigned):
    length = unassigned.shape[0]
    dma, anyspace = pltpu.SemaphoreType.DMA, pl.BlockSpec(memory_space=pl.ANY)
    vmem = pl.BlockSpec(memory_space=pltpu.VMEM)
    f32, bf16 = jnp.float32, jnp.bfloat16
    new_prices, margins, count = pl.pallas_call(
        kernel,
        out_shape=(
            jax.ShapeDtypeStruct((1, HALF), f32),
            jax.ShapeDtypeStruct((1, length), f32),
            jax.ShapeDtypeStruct((1, 1), jnp.int32),
        ),
        in_specs=[anyspace] * 4,
        out_specs=(vmem, vmem, vmem),
        scratch_shapes=[
            pltpu.VMEM((length, WIDTH), bf16),
            pltpu.VMEM((HALF, WIDTH), bf16),
            pltpu.VMEM((1, length), jnp.int32),
            pltpu.VMEM((1, length), jnp.int32),
            pltpu.VMEM((BUSY, length), f32),
            pltpu.VMEM((2, GROUPS, BUSY, WIDTH), bf16),
            pltpu.VMEM((2, OWNERS, HALF, WIDTH), bf16),
            pltpu.VMEM((OWNERS, 1, 128), f32),
            pltpu.VMEM((OWNERS, HALF, 128), f32),
            pltpu.VMEM((GROUPS, 1, 128), f32),
            pltpu.VMEM((4, OWNERS, HALF, 256), f32),
            pltpu.VMEM((16, 2, 8, 128), f32),
            pltpu.VMEM((OWNERS, 1, 128), f32),
            pltpu.VMEM((OWNERS, 1, 128), f32),
            dma((5,)),
            dma((5,)), dma((5,)),
            dma((2, 5, 2, 3)), dma((2, 5, 2, 3)),
            dma((2, 5, 2, 4)), dma((2, 5, 2, 4)),
            dma((3, Z)), dma((3, Z)),
            dma((2, 4)), dma((2, 4)),
            dma((X, 2)), dma((X, 2)),
            dma((X, Y)), dma((X, Y)),
            dma((Z, C)), dma((Z, C)),
        ],
        compiler_params=pltpu.CompilerParams(collective_id=0, has_side_effects=True, vmem_limit_bytes=67043328),
    )(tokens, slot_embed, price_units.reshape(1, length), unassigned.reshape(1, length))
    return new_prices.reshape(HALF), margins.reshape(length), count.reshape(())


def solution(mesh):
    return jax.shard_map(
        on_device,
        mesh=mesh,
        in_specs=(P("dp", "mp"), P("dp", "mp"), P("dp"), P("dp")),
        out_specs=(P(("dp", "mp")), P("dp"), P()),
        check_vma=False,
    )
```

```python
import jax
import jax.numpy as jnp
from jax import lax
from jax.experimental import pallas as pl
from jax.experimental.pallas import tpu as pltpu
from jax.sharding import PartitionSpec as P

MESH = pl.DeviceIdType.MESH
X, Y, Z, C = 4, 4, 8, 2
BUSY = 128
HALF = 80
WIDTH = 512
GROUPS = 8
OWNERS = 16
OFFS = (0, -1, 1, 2)
KINDS = (0, 0, 0, 1, 1)
UNIT = 1.0 / 512.0
PLAN = (
    (1, 2, 0), (1, 2, 1), (1, 2, 2), (1, 1, 0, 0, 0, 0), (1, 1, 0, 0, 1, 0), (1, 1, 0, 1, 0, 0), (1, 1, 0, 2, 0, 0),
    (1, 1, 0, 3, 1, 0), (1, 1, 0, 4, 1, 0), (1, 2, 3), (1, 1, 0, 1, 1, 0), (1, 1, 0, 3, 0, 0), (1, 2, 4),
    (1, 1, 0, 2, 1, 0), (1, 1, 0, 4, 0, 0), (2,), (1, 0, 0, 0, 0, 0), (1, 0, 0, 0, 0, 1), (1, 0, 1, 0, 0, 0),
    (1, 0, 1, 0, 0, 1), (1, 0, 0, 0, 1, 1), (1, 0, 0, 0, 1, 0), (1, 0, 1, 0, 1, 1), (1, 0, 1, 0, 1, 0),
    (1, 0, 0, 1, 0, 0), (1, 0, 1, 1, 0, 0), (1, 0, 1, 1, 0, 1), (1, 0, 0, 1, 1, 1), (1, 0, 1, 1, 1, 1),
    (1, 0, 1, 1, 1, 0), (1, 0, 0, 1, 0, 1), (0, 2, 0), (1, 1, 1, 0, 0, 0), (1, 1, 1, 0, 1, 0), (0, 1, 0, 0, 0, 0),
    (0, 1, 0, 0, 1, 0), (1, 1, 0, 0, 0, 1), (1, 1, 0, 0, 1, 1), (1, 0, 0, 1, 1, 0), (0, 2, 1), (1, 1, 1, 1, 0, 0),
    (1, 1, 1, 1, 1, 0), (0, 1, 0, 1, 0, 0), (0, 1, 0, 3, 1, 0), (1, 1, 0, 1, 0, 1), (1, 1, 0, 3, 1, 1), (0, 2, 2),
    (1, 1, 1, 2, 0, 0), (1, 1, 1, 2, 1, 0), (0, 1, 0, 2, 0, 0), (0, 1, 0, 4, 1, 0), (1, 1, 0, 2, 0, 1),
    (1, 1, 0, 4, 1, 1), (0, 0, 0, 0, 0, 0), (0, 0, 0, 0, 0, 1), (1, 0, 0, 0, 0, 2), (1, 0, 0, 2, 0, 0),
    (1, 0, 0, 3, 0, 0), (0, 2, 3), (1, 1, 1, 3, 0, 0), (1, 1, 1, 3, 1, 0), (0, 1, 0, 1, 1, 0), (0, 1, 0, 3, 0, 0),
    (1, 1, 0, 3, 0, 1), (0, 2, 4), (1, 1, 1, 4, 0, 0), (1, 1, 1, 4, 1, 0), (0, 1, 0, 2, 1, 0), (0, 1, 0, 4, 0, 0),
    (1, 1, 0, 4, 0, 1), (0, 0, 1, 0, 0, 0), (1, 0, 1, 0, 0, 2), (1, 0, 1, 2, 0, 0), (1, 0, 1, 2, 0, 1),
    (1, 0, 0, 2, 0, 1), (0, 0, 0, 0, 1, 0), (0, 0, 0, 0, 1, 1), (1, 0, 0, 2, 1, 1), (1, 0, 0, 0, 1, 2),
    (1, 0, 0, 3, 1, 1), (1, 1, 0, 1, 1, 1), (0, 0, 1, 0, 0, 1), (0, 0, 1, 0, 1, 1), (1, 0, 1, 3, 0, 0),
    (1, 0, 1, 3, 0, 1), (1, 0, 1, 0, 1, 2), (1, 0, 1, 3, 1, 1), (1, 0, 1, 3, 1, 0), (1, 1, 0, 2, 1, 1), (3, 0),
    (0, 0, 1, 0, 1, 0), (1, 0, 1, 2, 1, 1), (1, 0, 1, 2, 1, 0), (0, 0, 1, 1, 0, 0), (0, 0, 1, 1, 1, 1),
    (1, 0, 1, 1, 0, 2), (1, 0, 0, 2, 1, 0), (0, 1, 1, 0, 0, 0), (0, 1, 1, 0, 1, 0), (1, 1, 1, 0, 0, 1),
    (1, 1, 1, 0, 1, 1), (0, 1, 0, 0, 0, 1), (0, 1, 0, 0, 1, 1), (1, 1, 0, 0, 0, 2), (1, 0, 1, 1, 1, 2),
    (1, 0, 0, 3, 0, 1), (0, 1, 1, 1, 1, 0), (1, 1, 1, 1, 1, 1), (0, 0, 0, 1, 0, 0), (0, 0, 0, 1, 1, 1),
    (0, 3, 1, 1, 0), (0, 1, 1, 1, 0, 0), (1, 1, 1, 1, 0, 1), (1, 0, 0, 3, 1, 0), (0, 1, 0, 1, 0, 1),
    (1, 1, 0, 1, 0, 2), (0, 1, 1, 2, 1, 0), (1, 1, 1, 2, 1, 1), (0, 1, 0, 3, 1, 1), (0, 1, 1, 3, 0, 0),
    (1, 1, 0, 3, 1, 2), (1, 1, 1, 3, 0, 1), (0, 0, 0, 0, 0, 2), (1, 0, 0, 4, 0, 0), (1, 0, 0, 4, 0, 1),
    (0, 1, 1, 4, 0, 0), (1, 1, 1, 4, 0, 1), (0, 1, 0, 4, 1, 1), (1, 1, 0, 4, 1, 2), (0, 1, 1, 3, 1, 0),
    (1, 1, 1, 3, 1, 1), (0, 1, 1, 2, 0, 0), (1, 1, 1, 2, 0, 1), (1, 0, 0, 1, 1, 2), (0, 0, 0, 2, 0, 0),
    (0, 1, 0, 2, 0, 1), (1, 1, 0, 2, 0, 2), (1, 0, 0, 1, 0, 2), (0, 0, 0, 0, 1, 2), (1, 0, 0, 4, 1, 1),
    (1, 0, 0, 4, 1, 0), (0, 0, 1, 0, 0, 2), (1, 0, 1, 4, 0, 0), (1, 0, 1, 4, 0, 1), (0, 1, 1, 4, 1, 0),
    (1, 1, 1, 4, 1, 1), (0, 0, 1, 2, 0, 0), (0, 0, 0, 3, 0, 0), (1, 1, 0, 0, 1, 2), (3, 7), (0, 0, 1, 0, 1, 2),
    (1, 0, 1, 4, 1, 1), (1, 0, 1, 4, 1, 0), (0, 1, 0, 3, 0, 1), (1, 1, 0, 3, 0, 2), (0, 1, 1, 0, 1, 1),
    (1, 1, 1, 0, 1, 2), (0, 0, 1, 3, 0, 0), (1, 0, 1, 3, 0, 2), (1, 0, 1, 2, 0, 2), (0, 0, 0, 2, 1, 1),
    (0, 1, 0, 4, 0, 1), (1, 1, 0, 4, 0, 2), (0, 1, 1, 1, 1, 1), (1, 1, 1, 1, 1, 2), (1, 0, 0, 2, 1, 2), (3, 1),
    (0, 0, 1, 2, 1, 1), (0, 0, 1, 3, 1, 1), (1, 0, 1, 2, 1, 2), (1, 0, 1, 3, 1, 2), (0, 1, 1, 2, 1, 1),
    (1, 1, 1, 2, 1, 2), (1, 0, 0, 2, 0, 2), (0, 0, 0, 3, 1, 1), (0, 1, 0, 1, 1, 1), (1, 1, 0, 1, 1, 2),
    (1, 0, 0, 3, 1, 2), (0, 1, 1, 3, 0, 1), (1, 1, 1, 3, 0, 2), (0, 1, 1, 0, 0, 1), (1, 1, 1, 0, 0, 2),
    (0, 3, 1, 3, 0), (1, 0, 0, 3, 0, 2), (0, 1, 0, 0, 0, 2), (1, 1, 0, 0, 0, 3), (0, 1, 0, 2, 1, 1),
    (1, 1, 0, 2, 1, 2), (0, 1, 1, 4, 0, 1), (1, 1, 1, 4, 0, 2), (0, 3, 1, 2, 0), (0, 1, 0, 3, 1, 2),
    (1, 1, 0, 3, 1, 3), (0, 0, 0, 4, 0, 0), (1, 0, 0, 4, 0, 2), (0, 1, 0, 4, 1, 2), (1, 1, 0, 4, 1, 3),
    (0, 1, 1, 1, 0, 1), (1, 1, 1, 1, 0, 2), (0, 1, 0, 1, 0, 2), (1, 1, 0, 1, 0, 3), (0, 1, 1, 3, 1, 1),
    (1, 1, 1, 3, 1, 2), (0, 3, 1, 1, 1), (0, 0, 1, 4, 0, 0), (1, 0, 1, 4, 0, 2), (0, 0, 0, 4, 1, 1),
    (1, 0, 0, 4, 1, 2), (0, 1, 1, 4, 1, 1), (1, 1, 1, 4, 1, 2), (0, 1, 1, 2, 0, 1), (1, 1, 1, 2, 0, 2),
    (0, 1, 0, 2, 0, 2), (1, 1, 0, 2, 0, 3), (0, 1, 1, 0, 1, 2), (1, 1, 1, 0, 1, 3), (0, 0, 1, 4, 1, 1),
    (1, 0, 1, 4, 1, 2), (0, 3, 1, 4, 0), (0, 1, 1, 1, 1, 2), (1, 1, 1, 1, 1, 3), (0, 1, 1, 3, 0, 2),
    (1, 1, 1, 3, 0, 3), (0, 1, 1, 2, 1, 2), (1, 1, 1, 2, 1, 3), (3, 2), (3, 6), (0, 1, 1, 4, 0, 2),
    (1, 1, 1, 4, 0, 3), (0, 3, 0, 1, 0), (4, 2, 6, 0, 1, 7), (0, 4, 0, 0, 1), (0, 3, 1, 3, 1), (0, 3, 1, 2, 1),
    (0, 4, 0, 1, 0), (0, 3, 0, 2, 0), (4, 24, 25, 31), (0, 4, 0, 1, 1), (0, 3, 0, 4, 0), (0, 3, 0, 3, 0),
    (0, 3, 1, 4, 1), (0, 4, 1, 1, 1), (4, 9, 15, 10), (0, 4, 1, 0, 0), (0, 4, 0, 0, 0), (0, 4, 1, 1, 0),
    (0, 4, 1, 0, 1), (4, 23, 18, 22, 14, 16, 17), (3, 3), (4, 3, 11, 27, 26, 30, 8), (3, 4), (4, 19, 4, 12), (3, 5),
    (4, 13, 29, 21, 28, 20, 5),
)

def wrap(v, n):
    return lax.rem(v + n, n)


def merge(a1, a2, b1, b2):
    return jnp.maximum(a1, b1), jnp.maximum(jnp.minimum(a1, b1), jnp.maximum(a2, b2))


def kernel(
    tok_hbm, slot_hbm, unit_hbm, mask_hbm, price_out, margin_out, count_out,
    tok, give, units, mask, hot, bid, slt, prow, prep, flg, val, top, t2, sec, col, rz,
    lsem, sent, xr, br, zr, zl, sr, pr, fr, tr, cr,
):
    dp, yl = lax.axis_index("dp"), lax.axis_index("mp")
    c, yh = lax.rem(dp, 2), lax.rem(dp // 2, 2)
    z, x = lax.rem(dp // 4, Z), dp // 32
    y = yh * 2 + yl
    grp = x * 2 + yh

    def dev(x_, y_, z_, c_):
        return (((x_ * Z + z_) * 2 + y_ // 2) * 2 + c_, lax.rem(y_, 2))

    def send(src, dst, ssem, rsem, to):
        pltpu.make_async_remote_copy(
            src_ref=src, dst_ref=dst, send_sem=ssem, recv_sem=rsem, device_id=to, device_id_type=MESH
        ).start()

    def whole(ref, rsem, ssem=None):
        copy = pltpu.make_async_remote_copy(
            src_ref=ref, dst_ref=ref, send_sem=rsem if ssem is None else ssem, recv_sem=rsem,
            device_id=dev(x, y, z, 1 - c), device_id_type=MESH,
        )
        if ssem is None:
            copy.wait_recv()
        else:
            copy.wait_send()

    def far(d, n):
        return min(d, n - d)

    plane = [(dx, dy) for dx in range(X) for dy in range(Y) if dx or dy]
    plane.sort(key=lambda d: -far(d[0], X) - far(d[1], Y))
    column = [(dz, dc) for dz in range(Z) for dc in range(C) if dz or dc]
    column.sort(key=lambda d: -far(d[0], Z))

    def in_plane(dx, dy):
        return dev(wrap(x + dx, X), wrap(y + dy, Y), z, c)

    def in_column(dz, dc):
        return dev(x, y, wrap(z + dz, Z), wrap(c + dc, C))

    keep = pl.ds(pl.multiple_of(yl * HALF, 16), HALF)
    away = pl.ds(pl.multiple_of((1 - yl) * HALF, 16), HALF)
    loads = [
        pltpu.make_async_copy(mask_hbm, mask, lsem.at[0]),
        pltpu.make_async_copy(slot_hbm.at[away], give, lsem.at[1]),
        pltpu.make_async_copy(slot_hbm.at[keep], slt.at[yl, c], lsem.at[2]),
        pltpu.make_async_copy(tok_hbm, tok, lsem.at[3]),
        pltpu.make_async_copy(unit_hbm, units, lsem.at[4]),
    ]
    for load in loads:
        load.start()
    barrier = pltpu.get_barrier_semaphore()
    near = [in_plane(1, 0), in_plane(-1, 0), in_plane(0, 1), in_plane(0, -1)]
    near += [in_column(1, 0), in_column(-1, 0), in_column(0, 1)]
    for to in near:
        pl.semaphore_signal(barrier, inc=1, device_id=to, device_id_type=MESH)
    lanes = lax.broadcasted_iota(jnp.int32, (1, BUSY), 1)
    sub = lax.broadcasted_iota(jnp.int32, (8, 128), 0)
    length = mask.shape[1]

    def spread(chunk):
        prep[chunk] = jnp.broadcast_to(prow[chunk], (128, 128)).T[0:HALF, :]

    loads[4].wait()
    both = units[...].astype(jnp.float32) * UNIT
    mine = jnp.where(yl == 0, both[:, 0:HALF], both[:, HALF : 2 * HALF])
    prow[c] = jnp.concatenate([mine, jnp.zeros((1, 128 - HALF), jnp.float32)], axis=1)

    def compact():
        loads[0].wait()
        live = mask[...]
        before = lax.broadcasted_iota(jnp.int32, (length, length), 0) <= lax.broadcasted_iota(
            jnp.int32, (length, length), 1
        )
        live8 = jnp.broadcast_to(live.astype(jnp.float32), (8, length))
        rank = jnp.dot(
            live8.astype(jnp.bfloat16),
            before.astype(jnp.float32).astype(jnp.bfloat16),
            preferred_element_type=jnp.float32,
        )
        rank = jnp.where(live8 > 0, rank, 0.0)[0:1, :]
        places = lax.broadcasted_iota(jnp.int32, (BUSY, length), 0).astype(jnp.float32) + 1.0
        hot[...] = jnp.where(places == rank, 1.0, 0.0)
        total = jnp.sum(live.astype(jnp.float32), axis=1, keepdims=True)
        flg[grp] = jnp.where(lanes.astype(jnp.float32) < total, 1.0, 0.0)
        loads[3].wait()
        picked = jnp.dot(hot[...].astype(jnp.bfloat16), tok[...], preferred_element_type=jnp.float32)
        for k in range(WIDTH // 128):
            bid[yl, 0, yh, k * 128 : k * 128 + 128] = picked[:, k * 128 : k * 128 + 128].T.astype(jnp.bfloat16)

    loads[1].wait()
    loads[2].wait()
    pl.semaphore_wait(barrier, len(near))
    halves = (yl, 1 - yl)

    def rows_of(t, off, core, p=None):
        chunk = (halves[t], (off % Z) * 2 + core)
        return slt.at[chunk] if p is None else slt.at[chunk + (pl.ds(p * 16, 16),)]

    def piece(dx, dy, part, p):
        ya = wrap(y + dy, Y)
        return bid.at[lax.rem(ya, 2), dx % X, ya // 2, pl.ds(part * 256 + p * 128, 128)]

    def b_at(part, j, k):
        along_x = (part == 0) == (j == 0)
        off = 0 if j == 0 else OFFS[j - 1]
        dx, dy = (off, 0) if part == 0 else (0, off)
        return dx + (k if along_x else 0), dy + (0 if along_x else k), along_x

    def b_sem(part, j, p, kind):
        if j == 0:
            return br.at[part, p * 3 + kind]
        last = 3 if part == 1 and kind == 2 else 2
        return br.at[part, 2 + j * 4 + (p if kind == p else last)]

    def b_send(part, j, p, kind):
        k = (1, -1, 1 if p == 0 else -1)[kind]
        dx, dy, along_x = b_at(part, j, -k if kind == 2 else 0)
        to = in_plane(k, 0) if along_x else in_plane(0, k)
        dst = piece(dx - k if along_x else dx, dy, part, p)
        send(piece(dx, dy, part, p), dst, sent.at[0], b_sem(part, j, p, kind), to)

    def b_take(part, j, p, kind):
        dx, dy, _ = b_at(part, j, (-1, 1, 2)[kind])
        whole(piece(dx, dy, part, p), b_sem(part, j, p, kind))

    def b_rest(part, j, far_):
        whole(bid.at[0, 0, 0, 0 : 512 if part == 0 else 256], br.at[part, 4 + j * 4 + far_])

    def sibling(t, off):
        send(rows_of(t, off, c), rows_of(t, off, c), sent.at[2], sr.at[off % Z], in_column(0, 1))

    def from_sibling(off):
        whole(slt.at[0, 0:2], sr.at[off % Z])

    left = {(t, off): 5 for t in (0, 1) for off in range(Z)}

    def landed(t, off, n=1):
        left[t, off % Z] -= n
        if left[t, off % Z] == 0:
            sibling(t, off)

    def reach(t, kind, way):
        return 4 if kind ^ t ^ way == 0 else 3

    def z_sem(t, p, way, k):
        last = k == reach(t, KINDS[p], way) - 1
        return zl.at[t, way, KINDS[p]] if last else zr.at[t, p, way, k]

    def z_send(t, p, way, k):
        step = 1 if way == 0 else -1
        src, dst = -step * k, -step * (k + 1)
        send(rows_of(t, src, c, p), rows_of(t, dst, c, p), sent.at[1], z_sem(t, p, way, k), in_column(step, 0))

    def pair(off):
        return prow.at[pl.ds((off % Z) * 2, 2)]

    def price_send(way, k):
        step = 1 if way == 0 else -1
        send(pair(-step * k), pair(-step * (k + 1)), sent.at[3], pr.at[way * 4 + k], in_column(step, 0))

    def price_take(way, k):
        off = -(k + 1) if way == 0 else k + 1
        whole(pair(off), pr.at[way * 4 + k])
        if k < (3, 2)[way]:
            price_send(way, k + 1)
        spread((off % Z) * 2)
        spread((off % Z) * 2 + 1)

    def z_take(t, p, way, k):
        off = -(k + 1) if way == 0 else k + 1
        whole(rows_of(t, off, c, p), z_sem(t, p, way, k))
        landed(t, off)
        if (t, p) == (0, 0):
            price_take(way, k)

    def z_rest(t, way, kind):
        n, k = KINDS.count(kind), reach(t, kind, way) - 1
        off = -(k + 1) if way == 0 else k + 1
        whole(rows_of(t, off, c).at[0 : n * 16], zl.at[t, way, kind])
        landed(t, off, n)
        if (t, kind) == (0, KINDS[0]):
            price_take(way, k)

    def x_send(p):
        rows = pl.ds(p * 16, 16)
        send(give.at[rows], slt.at[yl, c, rows], sent.at[1], xr.at[p], dev(x, yh * 2 + 1 - yl, z, c))

    def x_take(p):
        whole(rows_of(1, 0, c, p), xr.at[p])
        landed(1, 0)

    seen = set()

    def values(n, off):
        acc = None
        for h in range(2):
            part = jnp.dot(
                slt[h, off * 2 : off * 2 + 2].reshape(2 * HALF, WIDTH),
                jnp.concatenate([bid[h, n, 0], bid[h, n, 1]], axis=1),
                preferred_element_type=jnp.float32,
            )
            acc = part if acc is None else acc + part
        price = prep[off * 2 : off * 2 + 2].reshape(2 * HALF, 128)
        v = acc - jnp.concatenate([price, price], axis=1)
        val[n, off * 2 : off * 2 + 2] = v.reshape(2, HALF, 256)
        if n in seen:
            m1, m2, first = top[n, 0], top[n, 1], 0
        else:
            m1, m2, first = v[0:8, :], jnp.full((8, 256), -jnp.inf, jnp.float32), 1
            seen.add(n)
        for r in range(first, 2 * HALF // 8):
            row = v[r * 8 : r * 8 + 8, :]
            m2 = jnp.maximum(m2, jnp.minimum(m1, row))
            m1 = jnp.maximum(m1, row)
        top[n, 0] = m1
        top[n, 1] = m2

    takes, sends = (b_take, z_take, x_take, b_rest, z_rest), (b_send, z_send, x_send)
    flag_at = max(i for i, op in enumerate(PLAN) if op[:2] in ((0, 0), (0, 3)))
    price_at = min(i for i, op in enumerate(PLAN) if op[0] == 0) - 1
    for i, op in enumerate(PLAN):
        if op[0] == 2:
            send(prow.at[c], prow.at[c], sent.at[3], pr.at[7], in_column(0, 1))
            sibling(0, 0)
            compact()
        elif op[0] == 3:
            from_sibling(op[1])
        elif op[0] == 4:
            for unit in op[1:]:
                values(unit // 8, unit % 8)
        else:
            (takes, sends)[op[0]][op[1]](*op[2:])
        if i == price_at:
            whole(prow.at[1 - c], pr.at[7])
            for way in (0, 1):
                price_send(way, 0)
            spread(0)
            spread(1)
        if i == flag_at:
            for dx in range(X):
                for dh in range(2):
                    if dx or dh:
                        send(flg.at[grp], flg.at[grp], sent.at[4], fr, in_plane(dx, 2 * dh))
    firsts, seconds = [], []
    for n in range(4):
        m1, m2 = top[n, 0], top[n, 1]
        for shift in (4, 2, 1):
            m1, m2 = merge(m1, m2, pltpu.roll(m1, shift, 0), pltpu.roll(m2, shift, 0))
        firsts += [m1[:, 0:128], m1[:, 128:256]]
        seconds += [m2[:, 0:128], m2[:, 128:256]]

    def group(dx, yh_):
        return wrap(x + dx, X) * 2 + yh_

    f, s2 = firsts[0], seconds[0]
    for i in range(GROUPS):
        f = jnp.where(sub == group(i // 2, i % 2), firsts[i], f)
        s2 = jnp.where(sub == group(i // 2, i % 2), seconds[i], s2)
    q = x * 4 + y
    t2[q, 0] = f
    t2[q, 1] = s2
    for dx, dy in plane:
        send(t2.at[q], t2.at[q], sent.at[5], tr, in_plane(dx, dy))
    whole(flg.at[0 : GROUPS - 1], fr)
    bidders = flg[0]
    for g in range(1, GROUPS):
        bidders = bidders + flg[g]
    bidders = jnp.sum(bidders, axis=1, keepdims=True)
    whole(t2.at[0:15], tr)
    f, s2 = t2[0, 0], t2[0, 1]
    for i in range(1, 16):
        f, s2 = merge(f, s2, t2[i, 0], t2[i, 1])
    sec[...] = s2
    bars = []
    for i in range(GROUPS):
        g = group(i // 2, i % 2)
        bars.append(jnp.broadcast_to(jnp.where(flg[g] > 0, sec[pl.ds(g, 1), :], jnp.inf), (HALF, 128)))
    for s in range(OWNERS):
        most_ = jnp.full((HALF, 128), -jnp.inf, jnp.float32)
        for i in range(GROUPS):
            most_ = jnp.maximum(most_, val[i // 2, s, :, (i % 2) * 128 : (i % 2) * 128 + 128] - bars[i])
        row = jnp.max(most_.T, axis=0, keepdims=True)
        row = jnp.concatenate([row, jnp.zeros((1, 128 - HALF), jnp.float32)], axis=1)
        col[s] = jnp.where(lanes == 127, bidders, row)
    for dz, dc in column:
        send(
            col.at[dz * 2 + wrap(c + dc, C)], rz.at[((Z - dz) % Z) * 2 + c], sent.at[6], cr, in_column(dz, dc)
        )
    rz[c] = col[c]
    gap = jnp.where(flg[grp] > 0, jnp.max(jnp.where(sub == grp, f - s2, -jnp.inf), axis=0, keepdims=True), 0.0)
    margin_out[...] = jnp.dot(
        jnp.broadcast_to(gap, (8, 128)), hot[...], precision=lax.Precision.HIGHEST, preferred_element_type=jnp.float32
    )[0:1, :]
    for i, ref in enumerate((val.at[0:3, 0:8], val.at[0, 0:15], val.at[0], rz.at[0:15], flg.at[0:7], t2.at[0:15])):
        whole(ref, sent.at[i], sent.at[i])
    whole(rz.at[0:15], cr)
    best, count = rz[0], rz[0]
    for i in range(1, OWNERS):
        best = jnp.maximum(best, rz[i])
        count = count + rz[i]
    price_out[...] = (prow[c] + jnp.maximum(best, 0.0))[:, 0:HALF]
    count_out[...] = count[:, 127:128].astype(jnp.int32)
    whole(rz.at[0:15], sent.at[6], sent.at[6])


def on_device(tokens, slot_embed, price_units, unassigned):
    length = unassigned.shape[0]
    dma, hbm = pltpu.SemaphoreType.DMA, pl.BlockSpec(memory_space=pltpu.HBM)
    vmem = pl.BlockSpec(memory_space=pltpu.VMEM)
    f32, bf16 = jnp.float32, jnp.bfloat16
    new_prices, margins, count = pl.pallas_call(
        kernel,
        out_shape=(
            jax.ShapeDtypeStruct((1, HALF), f32),
            jax.ShapeDtypeStruct((1, length), f32),
            jax.ShapeDtypeStruct((1, 1), jnp.int32),
        ),
        in_specs=[hbm] * 4,
        out_specs=(vmem, vmem, vmem),
        scratch_shapes=[
            pltpu.VMEM((length, WIDTH), bf16),
            pltpu.VMEM((HALF, WIDTH), bf16),
            pltpu.VMEM((1, length), jnp.int32),
            pltpu.VMEM((1, length), jnp.int32),
            pltpu.VMEM((BUSY, length), f32),
            pltpu.VMEM((2, X, 2, WIDTH, BUSY), bf16),
            pltpu.VMEM((2, OWNERS, HALF, WIDTH), bf16),
            pltpu.VMEM((OWNERS, 1, 128), f32),
            pltpu.VMEM((OWNERS, HALF, 128), f32),
            pltpu.VMEM((GROUPS, 1, 128), f32),
            pltpu.VMEM((4, OWNERS, HALF, 256), f32),
            pltpu.VMEM((4, 2, 8, 256), f32),
            pltpu.VMEM((16, 2, 8, 128), f32),
            pltpu.VMEM((8, 128), f32),
            pltpu.VMEM((OWNERS, 1, 128), f32),
            pltpu.VMEM((OWNERS, 1, 128), f32),
            dma((5,)),
            dma((7,)),
            dma((5,)),
            dma((2, 22)),
            dma((2, 5, 2, 3)),
            dma((2, 2, 2)),
            dma((Z,)),
            dma((8,)),
            dma, dma, dma,
        ],
        compiler_params=pltpu.CompilerParams(collective_id=0, has_side_effects=True, vmem_limit_bytes=32 << 20),
    )(
        *(
            pltpu.with_memory_space_constraint(v, pltpu.HBM)
            for v in (tokens, slot_embed, price_units.reshape(1, length), unassigned.reshape(1, length))
        )
    )
    return new_prices.reshape(HALF), margins.reshape(length), count.reshape(())


def solution(mesh):
    return jax.shard_map(
        on_device,
        mesh=mesh,
        in_specs=(P("dp", "mp"), P("dp", "mp"), P("dp"), P("dp")),
        out_specs=(P(("dp", "mp")), P("dp"), P()),
        check_vma=False,
    )
```

```python
import jax
import jax.numpy as jnp
from jax import lax
from jax.experimental import pallas as pl
from jax.experimental.pallas import tpu as pltpu
from jax.sharding import PartitionSpec as P

MESH = pl.DeviceIdType.MESH
X, Y, Z, C = 4, 4, 8, 2
BUSY = 128
HALF = 80
WIDTH = 512
GROUPS = 8
OWNERS = 16
OFFS = (0, -1, 1, 2)
PIECES = ((0, 48, 0), (48, 32, 1))
UNIT = 1.0 / 512.0
PLAN = (
    (1, 2, 0), (1, 2, 1), (1, 1, 0, 0, 0, 0), (1, 1, 0, 0, 1, 0), (1, 1, 0, 1, 0, 0), (1, 1, 0, 1, 1, 0), (2,),
    (1, 0, 0, 0, 0, 0), (1, 0, 0, 0, 0, 1), (1, 0, 1, 0, 0, 0), (1, 0, 1, 0, 0, 1), (1, 0, 0, 0, 1, 1),
    (1, 0, 0, 0, 1, 0), (1, 0, 1, 0, 1, 1), (1, 0, 1, 0, 1, 0), (1, 0, 0, 1, 0, 0), (1, 0, 0, 1, 0, 1),
    (1, 0, 1, 1, 0, 0), (1, 0, 1, 1, 0, 1), (1, 0, 0, 1, 1, 1), (1, 0, 0, 1, 1, 0), (1, 0, 1, 1, 1, 1),
    (1, 0, 1, 1, 1, 0), (0, 2, 0), (1, 1, 1, 0, 0, 0), (1, 1, 1, 0, 1, 0), (0, 1, 0, 0, 0, 0), (0, 1, 0, 0, 1, 0),
    (1, 1, 0, 0, 0, 1), (1, 1, 0, 0, 1, 1), (0, 0, 0, 0, 0, 0), (0, 0, 0, 0, 0, 1), (1, 0, 0, 0, 0, 2),
    (1, 0, 0, 2, 0, 0), (1, 0, 0, 2, 0, 1), (1, 0, 0, 3, 0, 0), (1, 0, 0, 3, 0, 1), (0, 2, 1), (1, 1, 1, 1, 0, 0),
    (1, 1, 1, 1, 1, 0), (0, 1, 0, 1, 0, 0), (0, 1, 0, 1, 1, 0), (1, 1, 0, 1, 0, 1), (1, 1, 0, 1, 1, 1),
    (0, 0, 1, 0, 0, 0), (1, 0, 1, 0, 0, 2), (1, 0, 1, 2, 0, 0), (1, 0, 1, 2, 0, 1), (0, 0, 0, 0, 1, 0),
    (0, 0, 0, 0, 1, 1), (1, 0, 0, 2, 1, 1), (1, 0, 0, 2, 1, 0), (1, 0, 0, 0, 1, 2), (1, 0, 0, 3, 1, 1),
    (1, 0, 0, 3, 1, 0), (0, 0, 1, 0, 0, 1), (0, 0, 1, 0, 1, 1), (1, 0, 1, 3, 0, 0), (1, 0, 1, 3, 0, 1),
    (1, 0, 1, 0, 1, 2), (1, 0, 1, 3, 1, 1), (1, 0, 1, 3, 1, 0), (3, 0), (0, 0, 1, 0, 1, 0), (1, 0, 1, 2, 1, 1),
    (1, 0, 1, 2, 1, 0), (0, 0, 1, 1, 0, 0), (0, 0, 1, 1, 1, 1), (1, 0, 1, 1, 0, 2), (1, 0, 1, 1, 1, 2),
    (0, 0, 0, 1, 0, 0), (0, 0, 0, 1, 1, 1), (1, 0, 0, 1, 0, 2), (1, 0, 0, 1, 1, 2), (0, 3, 1, 1, 0),
    (0, 0, 0, 0, 0, 2), (1, 0, 0, 4, 0, 0), (1, 0, 0, 4, 0, 1), (0, 0, 0, 2, 0, 0), (1, 0, 0, 2, 0, 2),
    (0, 1, 1, 0, 1, 0), (1, 1, 1, 0, 1, 1), (0, 1, 1, 1, 0, 0), (1, 1, 1, 1, 0, 1), (0, 1, 1, 0, 0, 0),
    (1, 1, 1, 0, 0, 1), (0, 0, 0, 3, 0, 0), (1, 0, 0, 3, 0, 2), (0, 0, 1, 0, 0, 2), (1, 0, 1, 4, 0, 0),
    (1, 0, 1, 4, 0, 1), (0, 0, 1, 2, 0, 0), (1, 0, 1, 2, 0, 2), (0, 1, 0, 0, 0, 1), (1, 1, 0, 0, 0, 2),
    (0, 0, 0, 0, 1, 2), (1, 0, 0, 4, 1, 1), (1, 0, 0, 4, 1, 0), (0, 0, 1, 0, 1, 2), (1, 0, 1, 4, 1, 1),
    (1, 0, 1, 4, 1, 0), (0, 0, 1, 3, 0, 0), (1, 0, 1, 3, 0, 2), (0, 1, 0, 0, 1, 1), (1, 1, 0, 0, 1, 2),
    (0, 1, 1, 1, 1, 0), (1, 1, 1, 1, 1, 1), (3, 7), (0, 1, 0, 1, 1, 1), (1, 1, 0, 1, 1, 2), (0, 0, 1, 2, 1, 1),
    (0, 0, 1, 3, 1, 1), (1, 0, 1, 2, 1, 2), (1, 0, 1, 3, 1, 2), (0, 0, 0, 2, 1, 1), (1, 0, 0, 2, 1, 2),
    (0, 0, 0, 3, 1, 1), (1, 0, 0, 3, 1, 2), (0, 3, 1, 2, 0), (0, 3, 1, 3, 0), (0, 1, 0, 1, 0, 1), (1, 1, 0, 1, 0, 2),
    (3, 1), (0, 3, 1, 1, 1), (0, 3, 0, 1, 0), (4, 0, 1, 7), (0, 0, 0, 4, 0, 0), (1, 0, 0, 4, 0, 2),
    (0, 1, 1, 0, 1, 1), (1, 1, 1, 0, 1, 2), (0, 1, 1, 1, 0, 1), (1, 1, 1, 1, 0, 2), (0, 1, 1, 0, 0, 1),
    (1, 1, 1, 0, 0, 2), (0, 0, 1, 4, 0, 0), (1, 0, 1, 4, 0, 2), (0, 1, 0, 0, 0, 2), (1, 1, 0, 0, 0, 3),
    (0, 0, 0, 4, 1, 1), (1, 0, 0, 4, 1, 2), (0, 0, 1, 4, 1, 1), (1, 0, 1, 4, 1, 2), (0, 3, 1, 4, 0), (0, 4, 0, 1, 0),
    (3, 6), (0, 1, 1, 1, 1, 1), (1, 1, 1, 1, 1, 2), (0, 1, 0, 1, 1, 2), (1, 1, 0, 1, 1, 3), (0, 3, 0, 2, 0),
    (4, 6, 24, 25), (0, 3, 1, 2, 1), (0, 3, 1, 3, 1), (0, 3, 0, 3, 0), (0, 4, 0, 0, 1), (3, 2), (0, 1, 1, 0, 1, 2),
    (1, 1, 1, 0, 1, 3), (0, 1, 1, 1, 0, 2), (1, 1, 1, 1, 0, 3), (4, 2, 10, 26, 9, 15, 14), (4, 31, 30, 8),
    (0, 3, 0, 4, 0), (0, 4, 1, 0, 0), (0, 3, 1, 4, 1), (0, 4, 0, 0, 0), (0, 4, 1, 1, 1), (4, 16, 17, 23),
    (0, 4, 0, 1, 1), (3, 3), (3, 5), (4, 5, 13, 29), (0, 4, 1, 0, 1), (0, 4, 1, 1, 0), (4, 11, 27, 19, 18, 22, 3),
    (3, 4), (4, 28, 20, 21, 4, 12),
)

def wrap(v, n):
    return lax.rem(v + n, n)


def merge(a1, a2, b1, b2):
    return jnp.maximum(a1, b1), jnp.maximum(jnp.minimum(a1, b1), jnp.maximum(a2, b2))


def kernel(
    tok_hbm, slot_hbm, unit_hbm, mask_hbm, price_out, margin_out, count_out,
    tok, give, units, mask, hot, bid, slt, prow, prep, flg, val, top, t2, sec, col, rz,
    lsem, sent, xr, br, zr, zl, sr, pr, fr, tr, cr,
):
    dp, yl = lax.axis_index("dp"), lax.axis_index("mp")
    c, yh = lax.rem(dp, 2), lax.rem(dp // 2, 2)
    z, x = lax.rem(dp // 4, Z), dp // 32
    y = yh * 2 + yl
    grp = x * 2 + yh

    def dev(x_, y_, z_, c_):
        return (((x_ * Z + z_) * 2 + y_ // 2) * 2 + c_, lax.rem(y_, 2))

    def send(src, dst, ssem, rsem, to):
        pltpu.make_async_remote_copy(
            src_ref=src, dst_ref=dst, send_sem=ssem, recv_sem=rsem, device_id=to, device_id_type=MESH
        ).start()

    def whole(ref, rsem, ssem=None):
        copy = pltpu.make_async_remote_copy(
            src_ref=ref, dst_ref=ref, send_sem=rsem if ssem is None else ssem, recv_sem=rsem,
            device_id=dev(x, y, z, 1 - c), device_id_type=MESH,
        )
        if ssem is None:
            copy.wait_recv()
        else:
            copy.wait_send()

    def far(d, n):
        return min(d, n - d)

    plane = [(dx, dy) for dx in range(X) for dy in range(Y) if dx or dy]
    plane.sort(key=lambda d: -far(d[0], X) - far(d[1], Y))
    column = [(dz, dc) for dz in range(Z) for dc in range(C) if dz or dc]
    column.sort(key=lambda d: -far(d[0], Z))

    def in_plane(dx, dy):
        return dev(wrap(x + dx, X), wrap(y + dy, Y), z, c)

    def in_column(dz, dc):
        return dev(x, y, wrap(z + dz, Z), wrap(c + dc, C))

    keep = pl.ds(pl.multiple_of(yl * HALF, 16), HALF)
    away = pl.ds(pl.multiple_of((1 - yl) * HALF, 16), HALF)
    loads = [
        pltpu.make_async_copy(mask_hbm, mask, lsem.at[0]),
        pltpu.make_async_copy(slot_hbm.at[away], give, lsem.at[1]),
        pltpu.make_async_copy(slot_hbm.at[keep], slt.at[yl, c], lsem.at[2]),
        pltpu.make_async_copy(tok_hbm, tok, lsem.at[3]),
        pltpu.make_async_copy(unit_hbm, units, lsem.at[4]),
    ]
    for load in loads:
        load.start()
    barrier = pltpu.get_barrier_semaphore()
    near = [in_plane(1, 0), in_plane(-1, 0), in_plane(0, 1), in_plane(0, -1)]
    near += [in_column(1, 0), in_column(-1, 0), in_column(0, 1)]
    for to in near:
        pl.semaphore_signal(barrier, inc=1, device_id=to, device_id_type=MESH)
    lanes = lax.broadcasted_iota(jnp.int32, (1, BUSY), 1)
    sub = lax.broadcasted_iota(jnp.int32, (8, 128), 0)
    length = mask.shape[1]

    def spread(chunk):
        prep[chunk] = jnp.broadcast_to(prow[chunk], (128, 128)).T[0:HALF, :]

    loads[4].wait()
    both = units[...].astype(jnp.float32) * UNIT
    mine = jnp.where(yl == 0, both[:, 0:HALF], both[:, HALF : 2 * HALF])
    prow[c] = jnp.concatenate([mine, jnp.zeros((1, 128 - HALF), jnp.float32)], axis=1)

    def compact():
        loads[0].wait()
        live = mask[...]
        before = lax.broadcasted_iota(jnp.int32, (length, length), 0) <= lax.broadcasted_iota(
            jnp.int32, (length, length), 1
        )
        live8 = jnp.broadcast_to(live.astype(jnp.float32), (8, length))
        rank = jnp.dot(
            live8.astype(jnp.bfloat16),
            before.astype(jnp.float32).astype(jnp.bfloat16),
            preferred_element_type=jnp.float32,
        )
        rank = jnp.where(live8 > 0, rank, 0.0)[0:1, :]
        places = lax.broadcasted_iota(jnp.int32, (BUSY, length), 0).astype(jnp.float32) + 1.0
        hot[...] = jnp.where(places == rank, 1.0, 0.0)
        total = jnp.sum(live.astype(jnp.float32), axis=1, keepdims=True)
        flg[grp] = jnp.where(lanes.astype(jnp.float32) < total, 1.0, 0.0)
        loads[3].wait()
        picked = jnp.dot(hot[...].astype(jnp.bfloat16), tok[...], preferred_element_type=jnp.float32)
        for k in range(WIDTH // 128):
            bid[yl, 0, yh, k * 128 : k * 128 + 128] = picked[:, k * 128 : k * 128 + 128].T.astype(jnp.bfloat16)

    loads[1].wait()
    loads[2].wait()
    pl.semaphore_wait(barrier, len(near))
    halves = (yl, 1 - yl)

    def rows_of(t, off, core, p=None):
        chunk = (halves[t], (off % Z) * 2 + core)
        return slt.at[chunk] if p is None else slt.at[chunk + (pl.ds(PIECES[p][0], PIECES[p][1]),)]

    def piece(dx, dy, part, p):
        ya = wrap(y + dy, Y)
        return bid.at[lax.rem(ya, 2), dx % X, ya // 2, pl.ds(part * 256 + p * 128, 128)]

    def b_at(part, j, k):
        along_x = (part == 0) == (j == 0)
        off = 0 if j == 0 else OFFS[j - 1]
        dx, dy = (off, 0) if part == 0 else (0, off)
        return dx + (k if along_x else 0), dy + (0 if along_x else k), along_x

    def b_sem(part, j, p, kind):
        if j == 0:
            return br.at[part, p * 3 + kind]
        last = 3 if part == 1 and kind == 2 else 2
        return br.at[part, 2 + j * 4 + (p if kind == p else last)]

    def b_send(part, j, p, kind):
        k = (1, -1, 1 if p == 0 else -1)[kind]
        dx, dy, along_x = b_at(part, j, -k if kind == 2 else 0)
        to = in_plane(k, 0) if along_x else in_plane(0, k)
        dst = piece(dx - k if along_x else dx, dy, part, p)
        send(piece(dx, dy, part, p), dst, sent.at[0], b_sem(part, j, p, kind), to)

    def b_take(part, j, p, kind):
        dx, dy, _ = b_at(part, j, (-1, 1, 2)[kind])
        whole(piece(dx, dy, part, p), b_sem(part, j, p, kind))

    def b_rest(part, j, far_):
        whole(bid.at[0, 0, 0, 0 : 512 if part == 0 else 256], br.at[part, 4 + j * 4 + far_])

    def sibling(t, off):
        send(rows_of(t, off, c), rows_of(t, off, c), sent.at[2], sr.at[off % Z], in_column(0, 1))

    def from_sibling(off):
        whole(slt.at[0, 0:2], sr.at[off % Z])

    left = {(t, off): len(PIECES) for t in (0, 1) for off in range(Z)}

    def landed(t, off, n=1):
        left[t, off % Z] -= n
        if left[t, off % Z] == 0:
            sibling(t, off)

    def reach(t, kind, way):
        return 4 if kind ^ t ^ way == 0 else 3

    def z_sem(t, p, way, k):
        last = k == reach(t, PIECES[p][2], way) - 1
        return zl.at[t, way, PIECES[p][2]] if last else zr.at[t, p, way, k]

    def z_send(t, p, way, k):
        step = 1 if way == 0 else -1
        src, dst = -step * k, -step * (k + 1)
        send(rows_of(t, src, c, p), rows_of(t, dst, c, p), sent.at[1], z_sem(t, p, way, k), in_column(step, 0))

    def pair(off):
        return prow.at[pl.ds((off % Z) * 2, 2)]

    def price_send(way, k):
        step = 1 if way == 0 else -1
        send(pair(-step * k), pair(-step * (k + 1)), sent.at[3], pr.at[way * 4 + k], in_column(step, 0))

    def price_take(way, k):
        off = -(k + 1) if way == 0 else k + 1
        whole(pair(off), pr.at[way * 4 + k])
        if k < (3, 2)[way]:
            price_send(way, k + 1)
        spread((off % Z) * 2)
        spread((off % Z) * 2 + 1)

    def z_take(t, p, way, k):
        off = -(k + 1) if way == 0 else k + 1
        whole(rows_of(t, off, c, p), z_sem(t, p, way, k))
        landed(t, off)
        if (t, p) == (0, 0):
            price_take(way, k)

    def z_rest(t, way, kind):
        mine, k = [p for p in PIECES if p[2] == kind], reach(t, kind, way) - 1
        off = -(k + 1) if way == 0 else k + 1
        whole(rows_of(t, off, c).at[0 : sum(p[1] for p in mine)], zl.at[t, way, kind])
        landed(t, off, len(mine))
        if (t, kind) == (0, PIECES[0][2]):
            price_take(way, k)

    def x_send(p):
        rows = pl.ds(PIECES[p][0], PIECES[p][1])
        send(give.at[rows], slt.at[yl, c, rows], sent.at[1], xr.at[p], dev(x, yh * 2 + 1 - yl, z, c))

    def x_take(p):
        whole(rows_of(1, 0, c, p), xr.at[p])
        landed(1, 0)

    seen = set()

    def values(n, off):
        acc = None
        for h in range(2):
            part = jnp.dot(
                slt[h, off * 2 : off * 2 + 2].reshape(2 * HALF, WIDTH),
                jnp.concatenate([bid[h, n, 0], bid[h, n, 1]], axis=1),
                preferred_element_type=jnp.float32,
            )
            acc = part if acc is None else acc + part
        price = prep[off * 2 : off * 2 + 2].reshape(2 * HALF, 128)
        v = acc - jnp.concatenate([price, price], axis=1)
        val[n, off * 2 : off * 2 + 2] = v.reshape(2, HALF, 256)
        if n in seen:
            m1, m2, first = top[n, 0], top[n, 1], 0
        else:
            m1, m2, first = v[0:8, :], jnp.full((8, 256), -jnp.inf, jnp.float32), 1
            seen.add(n)
        for r in range(first, 2 * HALF // 8):
            row = v[r * 8 : r * 8 + 8, :]
            m2 = jnp.maximum(m2, jnp.minimum(m1, row))
            m1 = jnp.maximum(m1, row)
        top[n, 0] = m1
        top[n, 1] = m2

    takes, sends = (b_take, z_take, x_take, b_rest, z_rest), (b_send, z_send, x_send)
    flag_at = max(i for i, op in enumerate(PLAN) if op[:2] in ((0, 0), (0, 3)))
    price_at = min(i for i, op in enumerate(PLAN) if op[0] == 0) - 1
    for i, op in enumerate(PLAN):
        if op[0] == 2:
            send(prow.at[c], prow.at[c], sent.at[3], pr.at[7], in_column(0, 1))
            sibling(0, 0)
            compact()
        elif op[0] == 3:
            from_sibling(op[1])
        elif op[0] == 4:
            for unit in op[1:]:
                values(unit // 8, unit % 8)
        else:
            (takes, sends)[op[0]][op[1]](*op[2:])
        if i == price_at:
            whole(prow.at[1 - c], pr.at[7])
            for way in (0, 1):
                price_send(way, 0)
            spread(0)
            spread(1)
        if i == flag_at:
            for dx in range(X):
                for dh in range(2):
                    if dx or dh:
                        send(flg.at[grp], flg.at[grp], sent.at[4], fr, in_plane(dx, 2 * dh))
    firsts, seconds = [], []
    for n in range(4):
        m1, m2 = top[n, 0], top[n, 1]
        for shift in (4, 2, 1):
            m1, m2 = merge(m1, m2, pltpu.roll(m1, shift, 0), pltpu.roll(m2, shift, 0))
        firsts += [m1[:, 0:128], m1[:, 128:256]]
        seconds += [m2[:, 0:128], m2[:, 128:256]]

    def group(dx, yh_):
        return wrap(x + dx, X) * 2 + yh_

    f, s2 = firsts[0], seconds[0]
    for i in range(GROUPS):
        f = jnp.where(sub == group(i // 2, i % 2), firsts[i], f)
        s2 = jnp.where(sub == group(i // 2, i % 2), seconds[i], s2)
    q = x * 4 + y
    t2[q, 0] = f
    t2[q, 1] = s2
    for dx, dy in plane:
        send(t2.at[q], t2.at[q], sent.at[5], tr, in_plane(dx, dy))
    whole(flg.at[0 : GROUPS - 1], fr)
    bidders = flg[0]
    for g in range(1, GROUPS):
        bidders = bidders + flg[g]
    bidders = jnp.sum(bidders, axis=1, keepdims=True)
    whole(t2.at[0:15], tr)
    f, s2 = t2[0, 0], t2[0, 1]
    for i in range(1, 16):
        f, s2 = merge(f, s2, t2[i, 0], t2[i, 1])
    sec[...] = s2
    bars = []
    for i in range(GROUPS):
        g = group(i // 2, i % 2)
        bars.append(jnp.broadcast_to(jnp.where(flg[g] > 0, sec[pl.ds(g, 1), :], jnp.inf), (HALF, 128)))
    for s in range(OWNERS):
        most_ = jnp.full((HALF, 128), -jnp.inf, jnp.float32)
        for i in range(GROUPS):
            most_ = jnp.maximum(most_, val[i // 2, s, :, (i % 2) * 128 : (i % 2) * 128 + 128] - bars[i])
        row = jnp.max(most_.T, axis=0, keepdims=True)
        row = jnp.concatenate([row, jnp.zeros((1, 128 - HALF), jnp.float32)], axis=1)
        col[s] = jnp.where(lanes == 127, bidders, row)
    for dz, dc in column:
        send(
            col.at[dz * 2 + wrap(c + dc, C)], rz.at[((Z - dz) % Z) * 2 + c], sent.at[6], cr, in_column(dz, dc)
        )
    rz[c] = col[c]
    gap = jnp.where(flg[grp] > 0, jnp.max(jnp.where(sub == grp, f - s2, -jnp.inf), axis=0, keepdims=True), 0.0)
    margin_out[...] = jnp.dot(
        jnp.broadcast_to(gap, (8, 128)), hot[...], precision=lax.Precision.HIGHEST, preferred_element_type=jnp.float32
    )[0:1, :]
    for i, ref in enumerate((val.at[0:3, 0:8], val.at[0, 0:15], val.at[0], rz.at[0:15], flg.at[0:7], t2.at[0:15])):
        whole(ref, sent.at[i], sent.at[i])
    whole(rz.at[0:15], cr)
    best, count = rz[0], rz[0]
    for i in range(1, OWNERS):
        best = jnp.maximum(best, rz[i])
        count = count + rz[i]
    price_out[...] = (prow[c] + jnp.maximum(best, 0.0))[:, 0:HALF]
    count_out[...] = count[:, 127:128].astype(jnp.int32)
    whole(rz.at[0:15], sent.at[6], sent.at[6])


def leave(*refs):
    copies = [pltpu.make_async_copy(refs[i], refs[3 + i], refs[6].at[i]) for i in range(3)]
    for copy in copies:
        copy.start()
    for copy in copies:
        copy.wait()


def on_device(tokens, slot_embed, price_units, unassigned):
    length = unassigned.shape[0]
    dma, hbm = pltpu.SemaphoreType.DMA, pl.BlockSpec(memory_space=pltpu.HBM)
    vmem = pl.BlockSpec(memory_space=pltpu.VMEM)
    f32, bf16 = jnp.float32, jnp.bfloat16
    new_prices, margins, count = pl.pallas_call(
        kernel,
        out_shape=(
            jax.ShapeDtypeStruct((1, HALF), f32),
            jax.ShapeDtypeStruct((1, length), f32),
            jax.ShapeDtypeStruct((1, 1), jnp.int32),
        ),
        in_specs=[hbm] * 4,
        out_specs=(vmem, vmem, vmem),
        scratch_shapes=[
            pltpu.VMEM((length, WIDTH), bf16),
            pltpu.VMEM((HALF, WIDTH), bf16),
            pltpu.VMEM((1, length), jnp.int32),
            pltpu.VMEM((1, length), jnp.int32),
            pltpu.VMEM((BUSY, length), f32),
            pltpu.VMEM((2, X, 2, WIDTH, BUSY), bf16),
            pltpu.VMEM((2, OWNERS, HALF, WIDTH), bf16),
            pltpu.VMEM((OWNERS, 1, 128), f32),
            pltpu.VMEM((OWNERS, HALF, 128), f32),
            pltpu.VMEM((GROUPS, 1, 128), f32),
            pltpu.VMEM((4, OWNERS, HALF, 256), f32),
            pltpu.VMEM((4, 2, 8, 256), f32),
            pltpu.VMEM((16, 2, 8, 128), f32),
            pltpu.VMEM((8, 128), f32),
            pltpu.VMEM((OWNERS, 1, 128), f32),
            pltpu.VMEM((OWNERS, 1, 128), f32),
            dma((5,)),
            dma((7,)),
            dma((len(PIECES),)),
            dma((2, 22)),
            dma((2, len(PIECES), 2, 3)),
            dma((2, 2, 2)),
            dma((Z,)),
            dma((8,)),
            dma, dma, dma,
        ],
        compiler_params=pltpu.CompilerParams(collective_id=0, has_side_effects=True, vmem_limit_bytes=32 << 20),
    )(
        *(
            pltpu.with_memory_space_constraint(v, pltpu.HBM)
            for v in (tokens, slot_embed, price_units.reshape(1, length), unassigned.reshape(1, length))
        )
    )
    new_prices, margins, count = pl.pallas_call(
        leave,
        out_shape=tuple(jax.ShapeDtypeStruct(v.shape, v.dtype) for v in (new_prices, margins, count)),
        in_specs=[vmem] * 3,
        out_specs=(hbm,) * 3,
        scratch_shapes=[dma((3,))],
        compiler_params=pltpu.CompilerParams(vmem_limit_bytes=1 << 20),
    )(new_prices, margins, count)
    return new_prices.reshape(HALF), margins.reshape(length), count.reshape(())


def solution(mesh):
    return jax.shard_map(
        on_device,
        mesh=mesh,
        in_specs=(P("dp", "mp"), P("dp", "mp"), P("dp"), P("dp")),
        out_specs=(P(("dp", "mp")), P("dp"), P()),
        check_vma=False,
    )
```

```python
import jax
import jax.numpy as jnp
from jax import lax
from jax.experimental import pallas as pl
from jax.experimental.pallas import tpu as pltpu
from jax.sharding import PartitionSpec as P

MESH = pl.DeviceIdType.MESH
X, Y, Z, C = 4, 4, 8, 2
BUSY = 128
HALF = 80
WIDTH = 512
GROUPS = 8
OWNERS = 16
OFFS = (0, -1, 1, 2)
PIECES = ((0, 48, 0), (48, 32, 1))
UNIT = 1.0 / 512.0
PLAN = (
    (1, 2, 0), (1, 2, 1), (1, 1, 0, 0, 0, 0), (1, 1, 0, 0, 1, 0), (1, 1, 0, 1, 0, 0), (1, 1, 0, 1, 1, 0), (2,),
    (1, 0, 0, 0, 0, 0), (1, 0, 0, 0, 0, 1), (1, 0, 1, 0, 0, 0), (1, 0, 1, 0, 0, 1), (1, 0, 0, 0, 1, 1),
    (1, 0, 0, 0, 1, 0), (1, 0, 1, 0, 1, 1), (1, 0, 1, 0, 1, 0), (1, 0, 0, 1, 0, 0), (1, 0, 0, 1, 0, 1),
    (1, 0, 1, 1, 0, 0), (1, 0, 1, 1, 0, 1), (1, 0, 0, 1, 1, 1), (1, 0, 0, 1, 1, 0), (1, 0, 1, 1, 1, 1),
    (1, 0, 1, 1, 1, 0), (0, 2, 0), (1, 1, 1, 0, 0, 0), (1, 1, 1, 0, 1, 0), (0, 1, 0, 0, 0, 0), (0, 1, 0, 0, 1, 0),
    (1, 1, 0, 0, 0, 1), (1, 1, 0, 0, 1, 1), (0, 0, 0, 0, 0, 0), (0, 0, 0, 0, 0, 1), (1, 0, 0, 0, 0, 2),
    (1, 0, 0, 2, 0, 0), (1, 0, 0, 2, 0, 1), (1, 0, 0, 3, 0, 0), (1, 0, 0, 3, 0, 1), (0, 2, 1), (1, 1, 1, 1, 0, 0),
    (1, 1, 1, 1, 1, 0), (0, 1, 0, 1, 0, 0), (0, 1, 0, 1, 1, 0), (1, 1, 0, 1, 0, 1), (1, 1, 0, 1, 1, 1),
    (0, 0, 1, 0, 0, 0), (1, 0, 1, 0, 0, 2), (1, 0, 1, 2, 0, 0), (1, 0, 1, 2, 0, 1), (0, 0, 0, 0, 1, 0),
    (0, 0, 0, 0, 1, 1), (1, 0, 0, 2, 1, 1), (1, 0, 0, 2, 1, 0), (1, 0, 0, 0, 1, 2), (1, 0, 0, 3, 1, 1),
    (1, 0, 0, 3, 1, 0), (0, 0, 1, 0, 0, 1), (0, 0, 1, 0, 1, 1), (1, 0, 1, 3, 0, 0), (1, 0, 1, 3, 0, 1),
    (1, 0, 1, 0, 1, 2), (1, 0, 1, 3, 1, 1), (1, 0, 1, 3, 1, 0), (3, 0), (0, 0, 1, 0, 1, 0), (1, 0, 1, 2, 1, 1),
    (1, 0, 1, 2, 1, 0), (0, 0, 1, 1, 0, 0), (0, 0, 1, 1, 1, 1), (1, 0, 1, 1, 0, 2), (1, 0, 1, 1, 1, 2),
    (0, 0, 0, 1, 0, 0), (0, 0, 0, 1, 1, 1), (1, 0, 0, 1, 0, 2), (1, 0, 0, 1, 1, 2), (0, 3, 1, 1, 0),
    (0, 0, 0, 0, 0, 2), (1, 0, 0, 4, 0, 0), (1, 0, 0, 4, 0, 1), (0, 0, 0, 2, 0, 0), (1, 0, 0, 2, 0, 2),
    (0, 1, 1, 0, 1, 0), (1, 1, 1, 0, 1, 1), (0, 1, 1, 1, 0, 0), (1, 1, 1, 1, 0, 1), (0, 1, 1, 0, 0, 0),
    (1, 1, 1, 0, 0, 1), (0, 0, 0, 3, 0, 0), (1, 0, 0, 3, 0, 2), (0, 0, 1, 0, 0, 2), (1, 0, 1, 4, 0, 0),
    (1, 0, 1, 4, 0, 1), (0, 0, 1, 2, 0, 0), (1, 0, 1, 2, 0, 2), (0, 1, 0, 0, 0, 1), (1, 1, 0, 0, 0, 2),
    (0, 0, 0, 0, 1, 2), (1, 0, 0, 4, 1, 1), (1, 0, 0, 4, 1, 0), (0, 0, 1, 0, 1, 2), (1, 0, 1, 4, 1, 1),
    (1, 0, 1, 4, 1, 0), (0, 0, 1, 3, 0, 0), (1, 0, 1, 3, 0, 2), (0, 1, 0, 0, 1, 1), (1, 1, 0, 0, 1, 2),
    (0, 1, 1, 1, 1, 0), (1, 1, 1, 1, 1, 1), (3, 7), (0, 1, 0, 1, 1, 1), (1, 1, 0, 1, 1, 2), (0, 0, 1, 2, 1, 1),
    (0, 0, 1, 3, 1, 1), (1, 0, 1, 2, 1, 2), (1, 0, 1, 3, 1, 2), (0, 0, 0, 2, 1, 1), (1, 0, 0, 2, 1, 2),
    (0, 0, 0, 3, 1, 1), (1, 0, 0, 3, 1, 2), (0, 3, 1, 2, 0), (0, 3, 1, 3, 0), (0, 1, 0, 1, 0, 1), (1, 1, 0, 1, 0, 2),
    (3, 1), (0, 3, 1, 1, 1), (0, 3, 0, 1, 0), (4, 0, 1, 7), (0, 0, 0, 4, 0, 0), (1, 0, 0, 4, 0, 2),
    (0, 1, 1, 0, 1, 1), (1, 1, 1, 0, 1, 2), (0, 1, 1, 1, 0, 1), (1, 1, 1, 1, 0, 2), (0, 1, 1, 0, 0, 1),
    (1, 1, 1, 0, 0, 2), (0, 0, 1, 4, 0, 0), (1, 0, 1, 4, 0, 2), (0, 1, 0, 0, 0, 2), (1, 1, 0, 0, 0, 3),
    (0, 0, 0, 4, 1, 1), (1, 0, 0, 4, 1, 2), (0, 0, 1, 4, 1, 1), (1, 0, 1, 4, 1, 2), (0, 3, 1, 4, 0), (0, 4, 0, 1, 0),
    (3, 6), (0, 1, 1, 1, 1, 1), (1, 1, 1, 1, 1, 2), (0, 1, 0, 1, 1, 2), (1, 1, 0, 1, 1, 3), (0, 3, 0, 2, 0),
    (4, 6, 24, 25), (0, 3, 1, 2, 1), (0, 3, 1, 3, 1), (0, 3, 0, 3, 0), (0, 4, 0, 0, 1), (3, 2), (0, 1, 1, 0, 1, 2),
    (1, 1, 1, 0, 1, 3), (0, 1, 1, 1, 0, 2), (1, 1, 1, 1, 0, 3), (4, 2, 10, 26, 9, 15, 14), (4, 31, 30, 8),
    (0, 3, 0, 4, 0), (0, 4, 1, 0, 0), (0, 3, 1, 4, 1), (0, 4, 0, 0, 0), (0, 4, 1, 1, 1), (4, 16, 17, 23),
    (0, 4, 0, 1, 1), (3, 3), (3, 5), (4, 5, 13, 29), (0, 4, 1, 0, 1), (0, 4, 1, 1, 0), (4, 11, 27, 19, 18, 22, 3),
    (3, 4), (4, 28, 20, 21, 4, 12),
)

def wrap(v, n):
    return lax.rem(v + n, n)


def merge(a1, a2, b1, b2):
    return jnp.maximum(a1, b1), jnp.maximum(jnp.minimum(a1, b1), jnp.maximum(a2, b2))


def kernel(
    tok_hbm, slot_hbm, unit_hbm, mask_hbm, price_out, margin_out, count_out,
    tok, give, units, mask, hot, bid, slt, prow, prep, flg, val, top, t2, sec, col, rz,
    lsem, sent, xr, br, zr, zl, sr, pr, fr, tr, cr,
):
    dp, yl = lax.axis_index("dp"), lax.axis_index("mp")
    c, yh = lax.rem(dp, 2), lax.rem(dp // 2, 2)
    z, x = lax.rem(dp // 4, Z), dp // 32
    y = yh * 2 + yl
    grp = x * 2 + yh

    def dev(x_, y_, z_, c_):
        return (((x_ * Z + z_) * 2 + y_ // 2) * 2 + c_, lax.rem(y_, 2))

    def send(src, dst, ssem, rsem, to):
        pltpu.make_async_remote_copy(
            src_ref=src, dst_ref=dst, send_sem=ssem, recv_sem=rsem, device_id=to, device_id_type=MESH
        ).start()

    def whole(ref, rsem, ssem=None):
        copy = pltpu.make_async_remote_copy(
            src_ref=ref, dst_ref=ref, send_sem=rsem if ssem is None else ssem, recv_sem=rsem,
            device_id=dev(x, y, z, 1 - c), device_id_type=MESH,
        )
        if ssem is None:
            copy.wait_recv()
        else:
            copy.wait_send()

    def far(d, n):
        return min(d, n - d)

    plane = [(dx, dy) for dx in range(X) for dy in range(Y) if dx or dy]
    plane.sort(key=lambda d: -far(d[0], X) - far(d[1], Y))
    column = [(dz, dc) for dz in range(Z) for dc in range(C) if dz or dc]
    column.sort(key=lambda d: -far(d[0], Z))

    def in_plane(dx, dy):
        return dev(wrap(x + dx, X), wrap(y + dy, Y), z, c)

    def in_column(dz, dc):
        return dev(x, y, wrap(z + dz, Z), wrap(c + dc, C))

    keep = pl.ds(pl.multiple_of(yl * HALF, 16), HALF)
    away = pl.ds(pl.multiple_of((1 - yl) * HALF, 16), HALF)
    loads = [
        pltpu.make_async_copy(mask_hbm, mask, lsem.at[0]),
        pltpu.make_async_copy(slot_hbm.at[away], give, lsem.at[1]),
        pltpu.make_async_copy(slot_hbm.at[keep], slt.at[yl, c], lsem.at[2]),
        pltpu.make_async_copy(tok_hbm, tok, lsem.at[3]),
        pltpu.make_async_copy(unit_hbm, units, lsem.at[4]),
    ]
    for load in loads:
        load.start()
    barrier = pltpu.get_barrier_semaphore()
    near = [in_plane(1, 0), in_plane(-1, 0), in_plane(0, 1), in_plane(0, -1)]
    near += [in_column(1, 0), in_column(-1, 0), in_column(0, 1)]
    for to in near:
        pl.semaphore_signal(barrier, inc=1, device_id=to, device_id_type=MESH)
    lanes = lax.broadcasted_iota(jnp.int32, (1, BUSY), 1)
    sub = lax.broadcasted_iota(jnp.int32, (8, 128), 0)
    length = mask.shape[1]

    def spread(chunk):
        prep[chunk] = jnp.broadcast_to(prow[chunk], (128, 128)).T[0:HALF, :]

    loads[4].wait()
    both = units[...].astype(jnp.float32) * UNIT
    mine = jnp.where(yl == 0, both[:, 0:HALF], both[:, HALF : 2 * HALF])
    prow[c] = jnp.concatenate([mine, jnp.zeros((1, 128 - HALF), jnp.float32)], axis=1)

    def compact():
        loads[0].wait()
        live = mask[...]
        before = lax.broadcasted_iota(jnp.int32, (length, length), 0) <= lax.broadcasted_iota(
            jnp.int32, (length, length), 1
        )
        live8 = jnp.broadcast_to(live.astype(jnp.float32), (8, length))
        rank = jnp.dot(
            live8.astype(jnp.bfloat16),
            before.astype(jnp.float32).astype(jnp.bfloat16),
            preferred_element_type=jnp.float32,
        )
        rank = jnp.where(live8 > 0, rank, 0.0)[0:1, :]
        places = lax.broadcasted_iota(jnp.int32, (BUSY, length), 0).astype(jnp.float32) + 1.0
        hot[...] = jnp.where(places == rank, 1.0, 0.0)
        total = jnp.sum(live.astype(jnp.float32), axis=1, keepdims=True)
        flg[grp] = jnp.where(lanes.astype(jnp.float32) < total, 1.0, 0.0)
        loads[3].wait()
        picked = jnp.dot(hot[...].astype(jnp.bfloat16), tok[...], preferred_element_type=jnp.float32)
        for k in range(WIDTH // 128):
            bid[yl, 0, yh, k * 128 : k * 128 + 128] = picked[:, k * 128 : k * 128 + 128].T.astype(jnp.bfloat16)

    loads[1].wait()
    loads[2].wait()
    pl.semaphore_wait(barrier, len(near))
    halves = (yl, 1 - yl)

    def rows_of(t, off, core, p=None):
        chunk = (halves[t], (off % Z) * 2 + core)
        return slt.at[chunk] if p is None else slt.at[chunk + (pl.ds(PIECES[p][0], PIECES[p][1]),)]

    def piece(dx, dy, part, p):
        ya = wrap(y + dy, Y)
        return bid.at[lax.rem(ya, 2), dx % X, ya // 2, pl.ds(part * 256 + p * 128, 128)]

    def b_at(part, j, k):
        along_x = (part == 0) == (j == 0)
        off = 0 if j == 0 else OFFS[j - 1]
        dx, dy = (off, 0) if part == 0 else (0, off)
        return dx + (k if along_x else 0), dy + (0 if along_x else k), along_x

    def b_sem(part, j, p, kind):
        if j == 0:
            return br.at[part, p * 3 + kind]
        last = 3 if part == 1 and kind == 2 else 2
        return br.at[part, 2 + j * 4 + (p if kind == p else last)]

    def b_send(part, j, p, kind):
        k = (1, -1, 1 if p == 0 else -1)[kind]
        dx, dy, along_x = b_at(part, j, -k if kind == 2 else 0)
        to = in_plane(k, 0) if along_x else in_plane(0, k)
        dst = piece(dx - k if along_x else dx, dy, part, p)
        send(piece(dx, dy, part, p), dst, sent.at[0], b_sem(part, j, p, kind), to)

    def b_take(part, j, p, kind):
        dx, dy, _ = b_at(part, j, (-1, 1, 2)[kind])
        whole(piece(dx, dy, part, p), b_sem(part, j, p, kind))

    def b_rest(part, j, far_):
        whole(bid.at[0, 0, 0, 0 : 512 if part == 0 else 256], br.at[part, 4 + j * 4 + far_])

    def sibling(t, off):
        send(rows_of(t, off, c), rows_of(t, off, c), sent.at[2], sr.at[off % Z], in_column(0, 1))

    def from_sibling(off):
        whole(slt.at[0, 0:2], sr.at[off % Z])

    left = {(t, off): len(PIECES) for t in (0, 1) for off in range(Z)}

    def landed(t, off, n=1):
        left[t, off % Z] -= n
        if left[t, off % Z] == 0:
            sibling(t, off)

    def reach(t, kind, way):
        return 4 if kind ^ t ^ way == 0 else 3

    def z_sem(t, p, way, k):
        last = k == reach(t, PIECES[p][2], way) - 1
        return zl.at[t, way, PIECES[p][2]] if last else zr.at[t, p, way, k]

    def z_send(t, p, way, k):
        step = 1 if way == 0 else -1
        src, dst = -step * k, -step * (k + 1)
        send(rows_of(t, src, c, p), rows_of(t, dst, c, p), sent.at[1], z_sem(t, p, way, k), in_column(step, 0))

    def pair(off):
        return prow.at[pl.ds((off % Z) * 2, 2)]

    def price_send(way, k):
        step = 1 if way == 0 else -1
        send(pair(-step * k), pair(-step * (k + 1)), sent.at[3], pr.at[way * 4 + k], in_column(step, 0))

    def price_take(way, k):
        off = -(k + 1) if way == 0 else k + 1
        whole(pair(off), pr.at[way * 4 + k])
        if k < (3, 2)[way]:
            price_send(way, k + 1)
        spread((off % Z) * 2)
        spread((off % Z) * 2 + 1)

    def z_take(t, p, way, k):
        off = -(k + 1) if way == 0 else k + 1
        whole(rows_of(t, off, c, p), z_sem(t, p, way, k))
        landed(t, off)
        if (t, p) == (0, 0):
            later.append((way, k))

    def z_rest(t, way, kind):
        mine, k = [p for p in PIECES if p[2] == kind], reach(t, kind, way) - 1
        off = -(k + 1) if way == 0 else k + 1
        whole(rows_of(t, off, c).at[0 : sum(p[1] for p in mine)], zl.at[t, way, kind])
        landed(t, off, len(mine))
        if (t, kind) == (0, PIECES[0][2]):
            later.append((way, k))

    def x_send(p):
        rows = pl.ds(PIECES[p][0], PIECES[p][1])
        send(give.at[rows], slt.at[yl, c, rows], sent.at[1], xr.at[p], dev(x, yh * 2 + 1 - yl, z, c))

    def x_take(p):
        whole(rows_of(1, 0, c, p), xr.at[p])
        landed(1, 0)

    seen = set()

    def values(n, off):
        acc = None
        for h in range(2):
            part = jnp.dot(
                slt[h, off * 2 : off * 2 + 2].reshape(2 * HALF, WIDTH),
                jnp.concatenate([bid[h, n, 0], bid[h, n, 1]], axis=1),
                preferred_element_type=jnp.float32,
            )
            acc = part if acc is None else acc + part
        price = prep[off * 2 : off * 2 + 2].reshape(2 * HALF, 128)
        v = acc - jnp.concatenate([price, price], axis=1)
        val[n, off * 2 : off * 2 + 2] = v.reshape(2, HALF, 256)
        if n in seen:
            m1, m2, first = top[n, 0], top[n, 1], 0
        else:
            m1, m2, first = v[0:8, :], jnp.full((8, 256), -jnp.inf, jnp.float32), 1
            seen.add(n)
        for r in range(first, 2 * HALF // 8):
            row = v[r * 8 : r * 8 + 8, :]
            m2 = jnp.maximum(m2, jnp.minimum(m1, row))
            m1 = jnp.maximum(m1, row)
        top[n, 0] = m1
        top[n, 1] = m2

    takes, sends = (b_take, z_take, x_take, b_rest, z_rest), (b_send, z_send, x_send)
    flag_at = max(i for i, op in enumerate(PLAN) if op[:2] in ((0, 0), (0, 3)))
    price_at = min(i for i, op in enumerate(PLAN) if op[0] == 0) - 1
    later = []
    for i, op in enumerate(PLAN):
        if op[0] != 1:
            while later and op[0] != 0:
                price_take(*later.pop(0))
        if op[0] == 2:
            send(prow.at[c], prow.at[c], sent.at[3], pr.at[7], in_column(0, 1))
            sibling(0, 0)
            compact()
        elif op[0] == 3:
            from_sibling(op[1])
        elif op[0] == 4:
            for unit in op[1:]:
                values(unit // 8, unit % 8)
        else:
            (takes, sends)[op[0]][op[1]](*op[2:])
        if len(later) > 1 and op[0] == 1 and PLAN[i + 1][0] != 1:
            price_take(*later.pop(0))
        if i == price_at:
            whole(prow.at[1 - c], pr.at[7])
            for way in (0, 1):
                price_send(way, 0)
            spread(0)
            spread(1)
        if i == flag_at:
            for dx in range(X):
                for dh in range(2):
                    if dx or dh:
                        send(flg.at[grp], flg.at[grp], sent.at[4], fr, in_plane(dx, 2 * dh))
    firsts, seconds = [], []
    for n in range(4):
        m1, m2 = top[n, 0], top[n, 1]
        for shift in (4, 2, 1):
            m1, m2 = merge(m1, m2, pltpu.roll(m1, shift, 0), pltpu.roll(m2, shift, 0))
        firsts += [m1[:, 0:128], m1[:, 128:256]]
        seconds += [m2[:, 0:128], m2[:, 128:256]]

    def group(dx, yh_):
        return wrap(x + dx, X) * 2 + yh_

    f, s2 = firsts[0], seconds[0]
    for i in range(GROUPS):
        f = jnp.where(sub == group(i // 2, i % 2), firsts[i], f)
        s2 = jnp.where(sub == group(i // 2, i % 2), seconds[i], s2)
    q = x * 4 + y
    t2[q, 0] = f
    t2[q, 1] = s2
    for dx, dy in plane:
        send(t2.at[q], t2.at[q], sent.at[5], tr, in_plane(dx, dy))
    whole(flg.at[0 : GROUPS - 1], fr)
    bidders = flg[0]
    for g in range(1, GROUPS):
        bidders = bidders + flg[g]
    bidders = jnp.sum(bidders, axis=1, keepdims=True)
    whole(t2.at[0:15], tr)
    f, s2 = t2[0, 0], t2[0, 1]
    for i in range(1, 16):
        f, s2 = merge(f, s2, t2[i, 0], t2[i, 1])
    sec[...] = s2
    bars = []
    for i in range(GROUPS):
        g = group(i // 2, i % 2)
        bars.append(jnp.broadcast_to(jnp.where(flg[g] > 0, sec[pl.ds(g, 1), :], jnp.inf), (HALF, 128)))
    for s in range(OWNERS):
        most_ = jnp.full((HALF, 128), -jnp.inf, jnp.float32)
        for i in range(GROUPS):
            most_ = jnp.maximum(most_, val[i // 2, s, :, (i % 2) * 128 : (i % 2) * 128 + 128] - bars[i])
        row = jnp.max(most_.T, axis=0, keepdims=True)
        row = jnp.concatenate([row, jnp.zeros((1, 128 - HALF), jnp.float32)], axis=1)
        col[s] = jnp.where(lanes == 127, bidders, row)
    for dz, dc in column:
        send(
            col.at[dz * 2 + wrap(c + dc, C)], rz.at[((Z - dz) % Z) * 2 + c], sent.at[6], cr, in_column(dz, dc)
        )
    rz[c] = col[c]
    for i, ref in enumerate((val.at[0:3, 0:8], val.at[0, 0:15], val.at[0], rz.at[0:15], flg.at[0:7], t2.at[0:15])):
        whole(ref, sent.at[i], sent.at[i])
    gap = jnp.where(flg[grp] > 0, jnp.max(jnp.where(sub == grp, f - s2, -jnp.inf), axis=0, keepdims=True), 0.0)
    margin_out[...] = jnp.dot(
        jnp.broadcast_to(gap, (8, 128)), hot[...], precision=lax.Precision.HIGHEST, preferred_element_type=jnp.float32
    )[0:1, :]
    whole(rz.at[0:15], sent.at[6], sent.at[6])
    whole(rz.at[0:15], cr)
    best, count = rz[0], rz[0]
    for i in range(1, OWNERS):
        best = jnp.maximum(best, rz[i])
        count = count + rz[i]
    price_out[...] = (prow[c] + jnp.maximum(best, 0.0))[:, 0:HALF]
    count_out[...] = count[:, 127:128].astype(jnp.int32)


def leave(*refs):
    copies = [pltpu.make_async_copy(refs[i], refs[3 + i], refs[6].at[i]) for i in range(3)]
    for copy in copies:
        copy.start()
    for copy in copies:
        copy.wait()


def on_device(tokens, slot_embed, price_units, unassigned):
    length = unassigned.shape[0]
    dma, hbm = pltpu.SemaphoreType.DMA, pl.BlockSpec(memory_space=pltpu.HBM)
    vmem = pl.BlockSpec(memory_space=pltpu.VMEM)
    f32, bf16 = jnp.float32, jnp.bfloat16
    new_prices, margins, count = pl.pallas_call(
        kernel,
        out_shape=(
            jax.ShapeDtypeStruct((1, HALF), f32),
            jax.ShapeDtypeStruct((1, length), f32),
            jax.ShapeDtypeStruct((1, 1), jnp.int32),
        ),
        in_specs=[hbm] * 4,
        out_specs=(vmem, vmem, vmem),
        scratch_shapes=[
            pltpu.VMEM((length, WIDTH), bf16),
            pltpu.VMEM((HALF, WIDTH), bf16),
            pltpu.VMEM((1, length), jnp.int32),
            pltpu.VMEM((1, length), jnp.int32),
            pltpu.VMEM((BUSY, length), f32),
            pltpu.VMEM((2, X, 2, WIDTH, BUSY), bf16),
            pltpu.VMEM((2, OWNERS, HALF, WIDTH), bf16),
            pltpu.VMEM((OWNERS, 1, 128), f32),
            pltpu.VMEM((OWNERS, HALF, 128), f32),
            pltpu.VMEM((GROUPS, 1, 128), f32),
            pltpu.VMEM((4, OWNERS, HALF, 256), f32),
            pltpu.VMEM((4, 2, 8, 256), f32),
            pltpu.VMEM((16, 2, 8, 128), f32),
            pltpu.VMEM((8, 128), f32),
            pltpu.VMEM((OWNERS, 1, 128), f32),
            pltpu.VMEM((OWNERS, 1, 128), f32),
            dma((5,)),
            dma((7,)),
            dma((len(PIECES),)),
            dma((2, 22)),
            dma((2, len(PIECES), 2, 3)),
            dma((2, 2, 2)),
            dma((Z,)),
            dma((8,)),
            dma, dma, dma,
        ],
        compiler_params=pltpu.CompilerParams(collective_id=0, has_side_effects=True, vmem_limit_bytes=32 << 20),
    )(
        *(
            pltpu.with_memory_space_constraint(v, pltpu.HBM)
            for v in (tokens, slot_embed, price_units.reshape(1, length), unassigned.reshape(1, length))
        )
    )
    new_prices, margins, count = pl.pallas_call(
        leave,
        out_shape=tuple(jax.ShapeDtypeStruct(v.shape, v.dtype) for v in (new_prices, margins, count)),
        in_specs=[vmem] * 3,
        out_specs=(hbm,) * 3,
        scratch_shapes=[dma((3,))],
        compiler_params=pltpu.CompilerParams(vmem_limit_bytes=1 << 20),
    )(new_prices, margins, count)
    return new_prices.reshape(HALF), margins.reshape(length), count.reshape(())


def solution(mesh):
    return jax.shard_map(
        on_device,
        mesh=mesh,
        in_specs=(P("dp", "mp"), P("dp", "mp"), P("dp"), P("dp")),
        out_specs=(P(("dp", "mp")), P("dp"), P()),
        check_vma=False,
    )
```

```python
import jax
import jax.numpy as jnp
from jax import lax
from jax.experimental import pallas as pl
from jax.experimental.pallas import tpu as pltpu
from jax.sharding import PartitionSpec as P

MESH = pl.DeviceIdType.MESH
X, Y, Z, C = 4, 4, 8, 2
BUSY = 128
HALF = 80
WIDTH = 512
GROUPS = 8
OWNERS = 16
OFFS = (0, -1, 1, 2)
PIECES = ((0, 48, 0), (48, 32, 1))
UNIT = 1.0 / 512.0
PLAN = (
    (1, 2, 0), (1, 2, 1), (1, 1, 0, 0, 0, 0), (1, 1, 0, 0, 1, 0), (1, 1, 0, 1, 0, 0), (1, 1, 0, 1, 1, 0), (2,),
    (1, 0, 0, 0, 0, 0), (1, 0, 0, 0, 0, 1), (1, 0, 1, 0, 0, 0), (1, 0, 1, 0, 0, 1), (1, 0, 0, 0, 1, 1),
    (1, 0, 0, 0, 1, 0), (1, 0, 1, 0, 1, 1), (1, 0, 1, 0, 1, 0), (1, 0, 0, 1, 0, 0), (1, 0, 0, 1, 0, 1),
    (1, 0, 1, 1, 0, 0), (1, 0, 1, 1, 0, 1), (1, 0, 0, 1, 1, 1), (1, 0, 0, 1, 1, 0), (1, 0, 1, 1, 1, 1),
    (1, 0, 1, 1, 1, 0), (0, 2, 0), (1, 1, 1, 0, 0, 0), (1, 1, 1, 0, 1, 0), (0, 1, 0, 0, 0, 0), (0, 1, 0, 0, 1, 0),
    (1, 1, 0, 0, 0, 1), (1, 1, 0, 0, 1, 1), (0, 0, 0, 0, 0, 0), (0, 0, 0, 0, 0, 1), (1, 0, 0, 0, 0, 2),
    (1, 0, 0, 2, 0, 0), (1, 0, 0, 2, 0, 1), (1, 0, 0, 3, 0, 0), (1, 0, 0, 3, 0, 1), (0, 2, 1), (1, 1, 1, 1, 0, 0),
    (1, 1, 1, 1, 1, 0), (0, 1, 0, 1, 0, 0), (0, 1, 0, 1, 1, 0), (1, 1, 0, 1, 0, 1), (1, 1, 0, 1, 1, 1),
    (0, 0, 1, 0, 0, 0), (1, 0, 1, 0, 0, 2), (1, 0, 1, 2, 0, 0), (1, 0, 1, 2, 0, 1), (0, 0, 0, 0, 1, 0),
    (0, 0, 0, 0, 1, 1), (1, 0, 0, 2, 1, 1), (1, 0, 0, 2, 1, 0), (1, 0, 0, 0, 1, 2), (1, 0, 0, 3, 1, 1),
    (1, 0, 0, 3, 1, 0), (0, 0, 1, 0, 0, 1), (0, 0, 1, 0, 1, 1), (1, 0, 1, 3, 0, 0), (1, 0, 1, 3, 0, 1),
    (1, 0, 1, 0, 1, 2), (1, 0, 1, 3, 1, 1), (1, 0, 1, 3, 1, 0), (3, 0), (0, 0, 1, 0, 1, 0), (1, 0, 1, 2, 1, 1),
    (1, 0, 1, 2, 1, 0), (0, 0, 1, 1, 0, 0), (0, 0, 1, 1, 1, 1), (1, 0, 1, 1, 0, 2), (1, 0, 1, 1, 1, 2),
    (0, 0, 0, 1, 0, 0), (0, 0, 0, 1, 1, 1), (1, 0, 0, 1, 0, 2), (1, 0, 0, 1, 1, 2), (0, 3, 1, 1, 0),
    (0, 0, 0, 0, 0, 2), (1, 0, 0, 4, 0, 0), (1, 0, 0, 4, 0, 1), (0, 0, 0, 2, 0, 0), (1, 0, 0, 2, 0, 2),
    (0, 1, 1, 0, 1, 0), (1, 1, 1, 0, 1, 1), (0, 1, 1, 1, 0, 0), (1, 1, 1, 1, 0, 1), (0, 1, 1, 0, 0, 0),
    (1, 1, 1, 0, 0, 1), (0, 0, 0, 3, 0, 0), (1, 0, 0, 3, 0, 2), (0, 0, 1, 0, 0, 2), (1, 0, 1, 4, 0, 0),
    (1, 0, 1, 4, 0, 1), (0, 0, 1, 2, 0, 0), (1, 0, 1, 2, 0, 2), (0, 1, 0, 0, 0, 1), (1, 1, 0, 0, 0, 2),
    (0, 0, 0, 0, 1, 2), (1, 0, 0, 4, 1, 1), (1, 0, 0, 4, 1, 0), (0, 0, 1, 0, 1, 2), (1, 0, 1, 4, 1, 1),
    (1, 0, 1, 4, 1, 0), (0, 0, 1, 3, 0, 0), (1, 0, 1, 3, 0, 2), (0, 1, 0, 0, 1, 1), (1, 1, 0, 0, 1, 2),
    (0, 1, 1, 1, 1, 0), (1, 1, 1, 1, 1, 1), (3, 7), (0, 1, 0, 1, 1, 1), (1, 1, 0, 1, 1, 2), (0, 0, 1, 2, 1, 1),
    (0, 0, 1, 3, 1, 1), (1, 0, 1, 2, 1, 2), (1, 0, 1, 3, 1, 2), (0, 0, 0, 2, 1, 1), (1, 0, 0, 2, 1, 2),
    (0, 0, 0, 3, 1, 1), (1, 0, 0, 3, 1, 2), (0, 3, 1, 2, 0), (0, 3, 1, 3, 0), (0, 1, 0, 1, 0, 1), (1, 1, 0, 1, 0, 2),
    (3, 1), (0, 3, 1, 1, 1), (0, 3, 0, 1, 0), (4, 0, 1, 7), (0, 0, 0, 4, 0, 0), (1, 0, 0, 4, 0, 2),
    (0, 1, 1, 0, 1, 1), (1, 1, 1, 0, 1, 2), (0, 1, 1, 1, 0, 1), (1, 1, 1, 1, 0, 2), (0, 1, 1, 0, 0, 1),
    (1, 1, 1, 0, 0, 2), (0, 0, 1, 4, 0, 0), (1, 0, 1, 4, 0, 2), (0, 1, 0, 0, 0, 2), (1, 1, 0, 0, 0, 3),
    (0, 0, 0, 4, 1, 1), (1, 0, 0, 4, 1, 2), (0, 0, 1, 4, 1, 1), (1, 0, 1, 4, 1, 2), (0, 3, 1, 4, 0), (0, 4, 0, 1, 0),
    (3, 6), (0, 1, 1, 1, 1, 1), (1, 1, 1, 1, 1, 2), (0, 1, 0, 1, 1, 2), (1, 1, 0, 1, 1, 3), (0, 3, 0, 2, 0),
    (4, 6, 24, 25), (0, 3, 1, 2, 1), (0, 3, 1, 3, 1), (0, 3, 0, 3, 0), (0, 4, 0, 0, 1), (3, 2), (0, 1, 1, 0, 1, 2),
    (1, 1, 1, 0, 1, 3), (0, 1, 1, 1, 0, 2), (1, 1, 1, 1, 0, 3), (4, 2, 10, 26, 9, 15, 14), (4, 31, 30, 8),
    (0, 3, 0, 4, 0), (0, 4, 1, 0, 0), (0, 3, 1, 4, 1), (0, 4, 0, 0, 0), (0, 4, 1, 1, 1), (4, 16, 17, 23),
    (0, 4, 0, 1, 1), (3, 3), (3, 5), (4, 5, 13, 29), (0, 4, 1, 0, 1), (0, 4, 1, 1, 0), (4, 11, 27, 19, 18, 22, 3),
    (3, 4), (4, 28, 20, 21, 4, 12),
)

def wrap(v, n):
    return lax.rem(v + n, n)


def merge(a1, a2, b1, b2):
    return jnp.maximum(a1, b1), jnp.maximum(jnp.minimum(a1, b1), jnp.maximum(a2, b2))


def kernel(
    tok_hbm, slot_hbm, unit_hbm, mask_hbm, price_out, margin_out, count_out,
    tok, give, units, mask, hot, bid, slt, prow, prep, flg, val, top, t2, sec, col, rz,
    lsem, sent, xr, br, zr, zl, sr, pr, fr, tr, cr,
):
    dp, yl = lax.axis_index("dp"), lax.axis_index("mp")
    c, yh = lax.rem(dp, 2), lax.rem(dp // 2, 2)
    z, x = lax.rem(dp // 4, Z), dp // 32
    y = yh * 2 + yl
    grp = x * 2 + yh

    def dev(x_, y_, z_, c_):
        return (((x_ * Z + z_) * 2 + y_ // 2) * 2 + c_, lax.rem(y_, 2))

    def send(src, dst, ssem, rsem, to):
        pltpu.make_async_remote_copy(
            src_ref=src, dst_ref=dst, send_sem=ssem, recv_sem=rsem, device_id=to, device_id_type=MESH
        ).start()

    def whole(ref, rsem, ssem=None):
        copy = pltpu.make_async_remote_copy(
            src_ref=ref, dst_ref=ref, send_sem=rsem if ssem is None else ssem, recv_sem=rsem,
            device_id=dev(x, y, z, 1 - c), device_id_type=MESH,
        )
        if ssem is None:
            copy.wait_recv()
        else:
            copy.wait_send()

    def far(d, n):
        return min(d, n - d)

    plane = [(dx, dy) for dx in range(X) for dy in range(Y) if dx or dy]
    plane.sort(key=lambda d: (-far(d[0], X) - far(d[1], Y), -far(d[1], Y)))
    column = [(dz, dc) for dz in range(Z) for dc in range(C) if dz or dc]
    column.sort(key=lambda d: -far(d[0], Z))

    def in_plane(dx, dy):
        return dev(wrap(x + dx, X), wrap(y + dy, Y), z, c)

    def in_column(dz, dc):
        return dev(x, y, wrap(z + dz, Z), wrap(c + dc, C))

    keep = pl.ds(pl.multiple_of(yl * HALF, 16), HALF)
    away = pl.ds(pl.multiple_of((1 - yl) * HALF, 16), HALF)
    loads = [
        pltpu.make_async_copy(mask_hbm, mask, lsem.at[0]),
        pltpu.make_async_copy(slot_hbm.at[away], give, lsem.at[1]),
        pltpu.make_async_copy(slot_hbm.at[keep], slt.at[yl, c], lsem.at[2]),
        pltpu.make_async_copy(tok_hbm, tok, lsem.at[3]),
        pltpu.make_async_copy(unit_hbm, units, lsem.at[4]),
    ]
    for load in loads:
        load.start()
    barrier = pltpu.get_barrier_semaphore()
    near = [in_plane(1, 0), in_plane(-1, 0), in_plane(0, 1), in_plane(0, -1)]
    near += [in_column(1, 0), in_column(-1, 0), in_column(0, 1)]
    for to in near:
        pl.semaphore_signal(barrier, inc=1, device_id=to, device_id_type=MESH)
    lanes = lax.broadcasted_iota(jnp.int32, (1, BUSY), 1)
    sub = lax.broadcasted_iota(jnp.int32, (8, 128), 0)
    length = mask.shape[1]

    def spread(chunk):
        prep[chunk] = jnp.broadcast_to(prow[chunk], (128, 128)).T[0:HALF, :]

    loads[4].wait()
    both = units[...].astype(jnp.float32) * UNIT
    mine = jnp.where(yl == 0, both[:, 0:HALF], both[:, HALF : 2 * HALF])
    prow[c] = jnp.concatenate([mine, jnp.zeros((1, 128 - HALF), jnp.float32)], axis=1)

    def compact():
        loads[0].wait()
        live = mask[...]
        before = lax.broadcasted_iota(jnp.int32, (length, length), 0) <= lax.broadcasted_iota(
            jnp.int32, (length, length), 1
        )
        live8 = jnp.broadcast_to(live.astype(jnp.float32), (8, length))
        rank = jnp.dot(
            live8.astype(jnp.bfloat16),
            before.astype(jnp.float32).astype(jnp.bfloat16),
            preferred_element_type=jnp.float32,
        )
        rank = jnp.where(live8 > 0, rank, 0.0)[0:1, :]
        places = lax.broadcasted_iota(jnp.int32, (BUSY, length), 0).astype(jnp.float32) + 1.0
        hot[...] = jnp.where(places == rank, 1.0, 0.0)
        total = jnp.sum(live.astype(jnp.float32), axis=1, keepdims=True)
        flg[grp] = jnp.where(lanes.astype(jnp.float32) < total, 1.0, 0.0)
        loads[3].wait()
        picked = jnp.dot(hot[...].astype(jnp.bfloat16), tok[...], preferred_element_type=jnp.float32)
        for k in range(WIDTH // 128):
            bid[yl, 0, yh, k * 128 : k * 128 + 128] = picked[:, k * 128 : k * 128 + 128].T.astype(jnp.bfloat16)

    loads[1].wait()
    loads[2].wait()
    pl.semaphore_wait(barrier, len(near))
    halves = (yl, 1 - yl)

    def rows_of(t, off, core, p=None):
        chunk = (halves[t], (off % Z) * 2 + core)
        return slt.at[chunk] if p is None else slt.at[chunk + (pl.ds(PIECES[p][0], PIECES[p][1]),)]

    def piece(dx, dy, part, p):
        ya = wrap(y + dy, Y)
        return bid.at[lax.rem(ya, 2), dx % X, ya // 2, pl.ds(part * 256 + p * 128, 128)]

    def b_at(part, j, k):
        along_x = (part == 0) == (j == 0)
        off = 0 if j == 0 else OFFS[j - 1]
        dx, dy = (off, 0) if part == 0 else (0, off)
        return dx + (k if along_x else 0), dy + (0 if along_x else k), along_x

    def b_sem(part, j, p, kind):
        if j == 0:
            return br.at[part, p * 3 + kind]
        last = 3 if part == 1 and kind == 2 else 2
        return br.at[part, 2 + j * 4 + (p if kind == p else last)]

    def b_send(part, j, p, kind):
        k = (1, -1, 1 if p == 0 else -1)[kind]
        dx, dy, along_x = b_at(part, j, -k if kind == 2 else 0)
        to = in_plane(k, 0) if along_x else in_plane(0, k)
        dst = piece(dx - k if along_x else dx, dy, part, p)
        send(piece(dx, dy, part, p), dst, sent.at[0], b_sem(part, j, p, kind), to)

    def b_take(part, j, p, kind):
        dx, dy, _ = b_at(part, j, (-1, 1, 2)[kind])
        whole(piece(dx, dy, part, p), b_sem(part, j, p, kind))

    def b_rest(part, j, far_):
        whole(bid.at[0, 0, 0, 0 : 512 if part == 0 else 256], br.at[part, 4 + j * 4 + far_])

    def sibling(t, off):
        send(rows_of(t, off, c), rows_of(t, off, c), sent.at[2], sr.at[off % Z], in_column(0, 1))

    def from_sibling(off):
        whole(slt.at[0, 0:2], sr.at[off % Z])

    left = {(t, off): len(PIECES) for t in (0, 1) for off in range(Z)}

    def landed(t, off, n=1):
        left[t, off % Z] -= n
        if left[t, off % Z] == 0:
            sibling(t, off)

    def reach(t, kind, way):
        return 4 if kind ^ t ^ way == 0 else 3

    def z_sem(t, p, way, k):
        if k == reach(t, PIECES[p][2], way) - 1:
            return zl.at[t, way, PIECES[p][2]]
        return zl.at[2, t, p] if k == 2 else zr.at[t, p, way, k]

    def z_send(t, p, way, k):
        step = 1 if way == 0 else -1
        src, dst = -step * k, -step * (k + 1)
        send(rows_of(t, src, c, p), rows_of(t, dst, c, p), sent.at[1], z_sem(t, p, way, k), in_column(step, 0))

    def pair(off):
        return prow.at[pl.ds((off % Z) * 2, 2)]

    def price_send(way, k):
        step = 1 if way == 0 else -1
        send(pair(-step * k), pair(-step * (k + 1)), sent.at[3], pr.at[way * 4 + k], in_column(step, 0))

    def price_take(way, k):
        off = -(k + 1) if way == 0 else k + 1
        whole(pair(off), pr.at[way * 4 + k])
        if k < (3, 2)[way]:
            price_send(way, k + 1)
        spread((off % Z) * 2)
        spread((off % Z) * 2 + 1)

    def z_take(t, p, way, k):
        off = -(k + 1) if way == 0 else k + 1
        whole(rows_of(t, off, c, p), z_sem(t, p, way, k))
        landed(t, off)
        if (t, p) == (0, 0):
            later.append((way, k))

    def z_rest(t, way, kind):
        mine, k = [p for p in PIECES if p[2] == kind], reach(t, kind, way) - 1
        off = -(k + 1) if way == 0 else k + 1
        whole(rows_of(t, off, c).at[0 : sum(p[1] for p in mine)], zl.at[t, way, kind])
        landed(t, off, len(mine))
        if (t, kind) == (0, PIECES[0][2]):
            later.append((way, k))

    def x_send(p):
        rows = pl.ds(PIECES[p][0], PIECES[p][1])
        send(give.at[rows], slt.at[yl, c, rows], sent.at[1], xr.at[p], dev(x, yh * 2 + 1 - yl, z, c))

    def x_take(p):
        whole(rows_of(1, 0, c, p), xr.at[p])
        landed(1, 0)

    seen = set()

    def values(n, off):
        acc = None
        for h in range(2):
            part = jnp.dot(
                slt[h, off * 2 : off * 2 + 2].reshape(2 * HALF, WIDTH),
                jnp.concatenate([bid[h, n, 0], bid[h, n, 1]], axis=1),
                preferred_element_type=jnp.float32,
            )
            acc = part if acc is None else acc + part
        price = prep[off * 2 : off * 2 + 2].reshape(2 * HALF, 128)
        v = acc - jnp.concatenate([price, price], axis=1)
        val[n, off * 2 : off * 2 + 2] = v.reshape(2, HALF, 256)
        if n in seen:
            m1, m2, first = top[n, 0], top[n, 1], 0
        else:
            m1, m2, first = v[0:8, :], jnp.full((8, 256), -jnp.inf, jnp.float32), 1
            seen.add(n)
        for r in range(first, 2 * HALF // 8):
            row = v[r * 8 : r * 8 + 8, :]
            m2 = jnp.maximum(m2, jnp.minimum(m1, row))
            m1 = jnp.maximum(m1, row)
        top[n, 0] = m1
        top[n, 1] = m2

    takes, sends = (b_take, z_take, x_take, b_rest, z_rest), (b_send, z_send, x_send)
    flag_at = max(i for i, op in enumerate(PLAN) if op[:2] in ((0, 0), (0, 3)))
    price_at = min(i for i, op in enumerate(PLAN) if op[0] == 0) - 1
    later = []
    for i, op in enumerate(PLAN):
        if op[0] != 1:
            while later and op[0] != 0:
                price_take(*later.pop(0))
        if op[0] == 2:
            send(prow.at[c], prow.at[c], sent.at[3], pr.at[7], in_column(0, 1))
            sibling(0, 0)
            compact()
        elif op[0] == 3:
            from_sibling(op[1])
        elif op[0] == 4:
            for unit in op[1:]:
                values(unit // 8, unit % 8)
        else:
            (takes, sends)[op[0]][op[1]](*op[2:])
        if len(later) > 1 and op[0] == 1 and PLAN[i + 1][0] != 1:
            price_take(*later.pop(0))
        if i == price_at:
            whole(prow.at[1 - c], pr.at[7])
            for way in (0, 1):
                price_send(way, 0)
            spread(0)
            spread(1)
        if i == flag_at:
            for dx in range(X):
                for dh in range(2):
                    if dx or dh:
                        send(flg.at[grp], flg.at[grp], sent.at[4], fr, in_plane(dx, 2 * dh))
    firsts, seconds = [], []
    for n in range(4):
        m1, m2 = top[n, 0], top[n, 1]
        for shift in (4, 2, 1):
            m1, m2 = merge(m1, m2, pltpu.roll(m1, shift, 0), pltpu.roll(m2, shift, 0))
        firsts += [m1[:, 0:128], m1[:, 128:256]]
        seconds += [m2[:, 0:128], m2[:, 128:256]]

    def group(dx, yh_):
        return wrap(x + dx, X) * 2 + yh_

    f, s2 = firsts[0], seconds[0]
    for i in range(GROUPS):
        f = jnp.where(sub == group(i // 2, i % 2), firsts[i], f)
        s2 = jnp.where(sub == group(i // 2, i % 2), seconds[i], s2)
    q = x * 4 + y
    t2[q, 0] = f
    t2[q, 1] = s2
    for dx, dy in plane:
        send(t2.at[q], t2.at[q], sent.at[5], tr, in_plane(dx, dy))
    whole(flg.at[0 : GROUPS - 1], fr)
    bidders = flg[0]
    for g in range(1, GROUPS):
        bidders = bidders + flg[g]
    bidders = jnp.sum(bidders, axis=1, keepdims=True)
    whole(t2.at[0:15], tr)
    f, s2 = t2[0, 0], t2[0, 1]
    for i in range(1, 16):
        f, s2 = merge(f, s2, t2[i, 0], t2[i, 1])
    sec[...] = s2
    bars = []
    for i in range(GROUPS):
        g = group(i // 2, i % 2)
        bars.append(jnp.broadcast_to(jnp.where(flg[g] > 0, sec[pl.ds(g, 1), :], jnp.inf), (HALF, 128)))
    for s in range(OWNERS):
        most_ = jnp.full((HALF, 128), -jnp.inf, jnp.float32)
        for i in range(GROUPS):
            most_ = jnp.maximum(most_, val[i // 2, s, :, (i % 2) * 128 : (i % 2) * 128 + 128] - bars[i])
        row = jnp.max(most_.T, axis=0, keepdims=True)
        row = jnp.concatenate([row, jnp.zeros((1, 128 - HALF), jnp.float32)], axis=1)
        col[s] = jnp.where(lanes == 127, bidders, row)
    for dz, dc in column:
        send(
            col.at[dz * 2 + wrap(c + dc, C)], rz.at[((Z - dz) % Z) * 2 + c], sent.at[6], cr, in_column(dz, dc)
        )
    rz[c] = col[c]
    for i, ref in enumerate((val.at[0:3, 0:8], val.at[0, 0:15], val.at[0], rz.at[0:15], flg.at[0:7], t2.at[0:15])):
        whole(ref, sent.at[i], sent.at[i])
    gap = jnp.where(flg[grp] > 0, jnp.max(jnp.where(sub == grp, f - s2, -jnp.inf), axis=0, keepdims=True), 0.0)
    margin_out[...] = jnp.dot(
        jnp.broadcast_to(gap, (8, 128)), hot[...], precision=lax.Precision.HIGHEST, preferred_element_type=jnp.float32
    )[0:1, :]
    whole(rz.at[0:15], sent.at[6], sent.at[6])
    whole(rz.at[0:15], cr)
    best, count = rz[0], rz[0]
    for i in range(1, OWNERS):
        best = jnp.maximum(best, rz[i])
        count = count + rz[i]
    price_out[...] = (prow[c] + jnp.maximum(best, 0.0))[:, 0:HALF]
    count_out[...] = count[:, 127:128].astype(jnp.int32)


def leave(*refs):
    copies = [pltpu.make_async_copy(refs[i], refs[3 + i], refs[6].at[i]) for i in range(3)]
    for copy in copies:
        copy.start()
    for copy in copies:
        copy.wait()


def on_device(tokens, slot_embed, price_units, unassigned):
    length = unassigned.shape[0]
    dma, hbm = pltpu.SemaphoreType.DMA, pl.BlockSpec(memory_space=pltpu.HBM)
    vmem = pl.BlockSpec(memory_space=pltpu.VMEM)
    f32, bf16 = jnp.float32, jnp.bfloat16
    new_prices, margins, count = pl.pallas_call(
        kernel,
        out_shape=(
            jax.ShapeDtypeStruct((1, HALF), f32),
            jax.ShapeDtypeStruct((1, length), f32),
            jax.ShapeDtypeStruct((1, 1), jnp.int32),
        ),
        in_specs=[hbm] * 4,
        out_specs=(vmem, vmem, vmem),
        scratch_shapes=[
            pltpu.VMEM((length, WIDTH), bf16),
            pltpu.VMEM((HALF, WIDTH), bf16),
            pltpu.VMEM((1, length), jnp.int32),
            pltpu.VMEM((1, length), jnp.int32),
            pltpu.VMEM((BUSY, length), f32),
            pltpu.VMEM((2, X, 2, WIDTH, BUSY), bf16),
            pltpu.VMEM((2, OWNERS, HALF, WIDTH), bf16),
            pltpu.VMEM((OWNERS, 1, 128), f32),
            pltpu.VMEM((OWNERS, HALF, 128), f32),
            pltpu.VMEM((GROUPS, 1, 128), f32),
            pltpu.VMEM((4, OWNERS, HALF, 256), f32),
            pltpu.VMEM((4, 2, 8, 256), f32),
            pltpu.VMEM((16, 2, 8, 128), f32),
            pltpu.VMEM((8, 128), f32),
            pltpu.VMEM((OWNERS, 1, 128), f32),
            pltpu.VMEM((OWNERS, 1, 128), f32),
            dma((5,)),
            dma((7,)),
            dma((len(PIECES),)),
            dma((2, 22)),
            dma((2, len(PIECES), 2, 2)),
            dma((3, 2, 2)),
            dma((Z,)),
            dma((8,)),
            dma, dma, dma,
        ],
        compiler_params=pltpu.CompilerParams(collective_id=0, has_side_effects=True, vmem_limit_bytes=32 << 20),
    )(
        *(
            pltpu.with_memory_space_constraint(v, pltpu.HBM)
            for v in (tokens, slot_embed, price_units.reshape(1, length), unassigned.reshape(1, length))
        )
    )
    new_prices, margins, count = pl.pallas_call(
        leave,
        out_shape=tuple(jax.ShapeDtypeStruct(v.shape, v.dtype) for v in (new_prices, margins, count)),
        in_specs=[vmem] * 3,
        out_specs=(hbm,) * 3,
        scratch_shapes=[dma((3,))],
        compiler_params=pltpu.CompilerParams(vmem_limit_bytes=1 << 20),
    )(new_prices, margins, count)
    return new_prices.reshape(HALF), margins.reshape(length), count.reshape(())


def solution(mesh):
    return jax.shard_map(
        on_device,
        mesh=mesh,
        in_specs=(P("dp", "mp"), P("dp", "mp"), P("dp"), P("dp")),
        out_specs=(P(("dp", "mp")), P("dp"), P()),
        check_vma=False,
    )
```

```python
import jax
import jax.numpy as jnp
from jax import lax
from jax.experimental import pallas as pl
from jax.experimental.pallas import tpu as pltpu
from jax.sharding import PartitionSpec as P

MESH = pl.DeviceIdType.MESH
X, Y, Z, C = 4, 4, 8, 2
BUSY = 128
HALF = 80
WIDTH = 512
GROUPS = 8
OWNERS = 16
OFFS = (0, -1, 1, 2)
PIECES = ((0, 16, 0), (16, 16, 0), (32, 16, 0), (48, 16, 1), (64, 16, 1))
UNIT = 1.0 / 512.0
PLAN = (
    (1, 2, 0), (1, 1, 0, 0, 0, 0), (1, 1, 0, 0, 1, 0), (1, 2, 1), (1, 1, 0, 1, 0, 0), (1, 1, 0, 3, 1, 0), (1, 2, 2),
    (1, 1, 0, 2, 0, 0), (1, 1, 0, 4, 1, 0), (1, 2, 3), (1, 1, 0, 1, 1, 0), (1, 1, 0, 3, 0, 0), (1, 2, 4),
    (1, 1, 0, 2, 1, 0), (1, 1, 0, 4, 0, 0), (2,), (1, 0, 0, 0, 0, 0), (1, 0, 0, 0, 0, 1), (1, 0, 1, 0, 0, 0),
    (1, 0, 1, 0, 0, 1), (1, 0, 0, 0, 1, 1), (1, 0, 0, 0, 1, 0), (1, 0, 1, 0, 1, 1), (1, 0, 1, 0, 1, 0),
    (1, 0, 1, 1, 0, 0), (1, 0, 1, 1, 1, 1), (1, 0, 0, 1, 0, 0), (1, 0, 0, 1, 1, 1), (1, 0, 1, 1, 0, 1),
    (1, 0, 1, 1, 1, 0), (1, 0, 0, 1, 0, 1), (1, 0, 0, 1, 1, 0), (0, 2, 0), (1, 1, 1, 0, 0, 0), (1, 1, 1, 0, 1, 0),
    (0, 1, 0, 0, 0, 0), (0, 1, 0, 0, 1, 0), (1, 1, 0, 0, 0, 1), (1, 1, 0, 0, 1, 1), (0, 2, 1), (1, 1, 1, 1, 0, 0),
    (1, 1, 1, 1, 1, 0), (0, 1, 0, 1, 0, 0), (0, 1, 0, 3, 1, 0), (1, 1, 0, 1, 0, 1), (1, 1, 0, 3, 1, 1), (0, 2, 2),
    (1, 1, 1, 2, 1, 0), (0, 1, 0, 2, 0, 0), (0, 1, 0, 4, 1, 0), (1, 1, 0, 4, 1, 1), (0, 0, 0, 0, 0, 0),
    (0, 0, 0, 0, 0, 1), (1, 0, 0, 0, 0, 2), (1, 0, 0, 2, 0, 0), (1, 0, 0, 2, 0, 1), (1, 0, 0, 3, 0, 0), (0, 2, 3),
    (1, 1, 1, 3, 0, 0), (1, 1, 1, 3, 1, 0), (0, 1, 0, 1, 1, 0), (0, 1, 0, 3, 0, 0), (1, 1, 1, 2, 0, 0),
    (1, 0, 0, 3, 0, 1), (1, 1, 0, 2, 0, 1), (0, 2, 4), (1, 1, 1, 4, 0, 0), (0, 1, 0, 2, 1, 0), (0, 1, 0, 4, 0, 0),
    (1, 1, 1, 4, 1, 0), (0, 0, 1, 0, 0, 0), (1, 0, 1, 0, 0, 2), (1, 0, 1, 2, 0, 0), (1, 0, 1, 2, 0, 1),
    (0, 0, 0, 0, 1, 0), (0, 0, 0, 0, 1, 1), (1, 0, 0, 0, 1, 2), (1, 0, 0, 2, 1, 1), (1, 1, 0, 1, 1, 1),
    (1, 1, 0, 3, 0, 1), (0, 0, 1, 0, 0, 1), (0, 0, 1, 0, 1, 1), (1, 0, 1, 3, 0, 0), (1, 0, 1, 3, 0, 1),
    (1, 0, 1, 0, 1, 2), (1, 0, 1, 3, 1, 1), (1, 1, 0, 2, 1, 1), (1, 1, 0, 4, 0, 1), (1, 0, 0, 3, 1, 1),
    (1, 0, 0, 2, 1, 0), (3, 0), (0, 0, 1, 0, 1, 0), (1, 0, 1, 2, 1, 1), (0, 0, 1, 1, 0, 0), (0, 0, 1, 1, 1, 1),
    (1, 0, 1, 2, 1, 0), (1, 0, 1, 3, 1, 0), (1, 0, 0, 3, 1, 0), (0, 0, 0, 1, 0, 0), (0, 0, 0, 1, 1, 1),
    (0, 3, 1, 1, 0), (1, 0, 1, 1, 0, 2), (1, 0, 1, 1, 1, 2), (1, 0, 0, 1, 0, 2), (1, 0, 0, 1, 1, 2),
    (0, 1, 1, 0, 0, 0), (0, 1, 1, 0, 1, 0), (1, 1, 1, 0, 0, 1), (1, 1, 1, 0, 1, 1), (0, 1, 0, 0, 0, 1),
    (0, 1, 0, 0, 1, 1), (1, 1, 0, 0, 0, 2), (1, 1, 0, 0, 1, 2), (0, 1, 1, 1, 1, 0), (1, 1, 1, 1, 1, 1),
    (0, 1, 1, 1, 0, 0), (1, 1, 1, 1, 0, 1), (0, 1, 0, 1, 0, 1), (1, 1, 0, 1, 0, 2), (0, 1, 1, 2, 1, 0),
    (1, 1, 1, 2, 1, 1), (0, 1, 0, 3, 1, 1), (0, 1, 1, 3, 0, 0), (1, 1, 0, 3, 1, 2), (1, 1, 1, 3, 0, 1),
    (0, 0, 0, 0, 0, 2), (1, 0, 0, 4, 0, 0), (1, 0, 0, 4, 0, 1), (0, 0, 0, 2, 0, 0), (1, 0, 0, 2, 0, 2),
    (0, 1, 1, 4, 0, 0), (1, 1, 1, 4, 0, 1), (0, 1, 0, 4, 1, 1), (1, 1, 0, 4, 1, 2), (0, 1, 1, 3, 1, 0),
    (1, 1, 1, 3, 1, 1), (0, 1, 1, 2, 0, 0), (1, 1, 1, 2, 0, 1), (0, 0, 0, 3, 0, 0), (1, 0, 0, 3, 0, 2),
    (0, 0, 1, 0, 0, 2), (1, 0, 1, 4, 0, 0), (1, 0, 1, 4, 0, 1), (0, 1, 0, 2, 0, 1), (1, 1, 0, 2, 0, 2),
    (0, 0, 1, 2, 0, 0), (1, 0, 1, 2, 0, 2), (0, 1, 1, 4, 1, 0), (1, 1, 1, 4, 1, 1), (0, 0, 0, 0, 1, 2),
    (1, 0, 0, 4, 1, 1), (1, 0, 0, 4, 1, 0), (0, 0, 1, 0, 1, 2), (1, 0, 1, 4, 1, 1), (1, 0, 1, 4, 1, 0),
    (0, 0, 1, 3, 0, 0), (1, 0, 1, 3, 0, 2), (0, 1, 0, 1, 1, 1), (0, 1, 0, 3, 0, 1), (1, 1, 0, 1, 1, 2),
    (1, 1, 0, 3, 0, 2), (3, 1), (3, 7), (0, 0, 1, 2, 1, 1), (0, 0, 1, 3, 1, 1), (1, 0, 1, 2, 1, 2),
    (1, 0, 1, 3, 1, 2), (0, 0, 0, 2, 1, 1), (1, 0, 0, 2, 1, 2), (0, 1, 0, 2, 1, 1), (0, 1, 0, 4, 0, 1),
    (1, 1, 0, 2, 1, 2), (1, 1, 0, 4, 0, 2), (0, 0, 0, 3, 1, 1), (1, 0, 0, 3, 1, 2), (0, 1, 1, 0, 0, 1),
    (0, 1, 1, 0, 1, 1), (1, 1, 1, 0, 0, 2), (1, 1, 1, 0, 1, 2), (0, 3, 1, 2, 0), (0, 3, 1, 3, 0), (0, 1, 0, 0, 0, 2),
    (1, 1, 0, 0, 0, 3), (0, 1, 1, 1, 1, 1), (1, 1, 1, 1, 1, 2), (0, 1, 1, 1, 0, 1), (1, 1, 1, 1, 0, 2),
    (0, 1, 0, 1, 0, 2), (1, 1, 0, 1, 0, 3), (0, 3, 1, 1, 1), (0, 1, 1, 2, 1, 1), (1, 1, 1, 2, 1, 2), (0, 3, 0, 1, 0),
    (4, 0, 1, 7), (0, 1, 0, 3, 1, 2), (0, 1, 1, 3, 0, 1), (1, 1, 0, 3, 1, 3), (1, 1, 1, 3, 0, 2), (0, 1, 1, 4, 0, 1),
    (1, 1, 1, 4, 0, 2), (0, 1, 0, 4, 1, 2), (1, 1, 0, 4, 1, 3), (0, 1, 1, 3, 1, 1), (1, 1, 1, 3, 1, 2),
    (0, 1, 1, 2, 0, 1), (1, 1, 1, 2, 0, 2), (0, 1, 0, 2, 0, 2), (1, 1, 0, 2, 0, 3), (0, 0, 0, 4, 0, 0),
    (1, 0, 0, 4, 0, 2), (0, 1, 1, 4, 1, 1), (1, 1, 1, 4, 1, 2), (0, 0, 1, 4, 0, 0), (1, 0, 1, 4, 0, 2), (3, 2),
    (3, 6), (4, 2, 6), (0, 4, 0, 1, 0), (0, 4, 0, 0, 1), (0, 0, 0, 4, 1, 1), (1, 0, 0, 4, 1, 2), (0, 0, 1, 4, 1, 1),
    (1, 0, 1, 4, 1, 2), (0, 3, 1, 4, 0), (0, 3, 0, 2, 0), (4, 24, 25, 31), (0, 1, 1, 0, 1, 2), (1, 1, 1, 0, 1, 3),
    (0, 3, 1, 2, 1), (0, 3, 1, 3, 1), (0, 3, 0, 3, 0), (4, 14), (0, 1, 1, 1, 1, 2), (1, 1, 1, 1, 1, 3),
    (0, 1, 1, 2, 1, 2), (1, 1, 1, 2, 1, 3), (0, 1, 1, 3, 0, 2), (1, 1, 1, 3, 0, 3), (0, 1, 1, 4, 0, 2),
    (1, 1, 1, 4, 0, 3), (4, 9, 15, 10, 26, 30, 8), (0, 4, 0, 1, 1), (0, 4, 1, 0, 0), (0, 4, 0, 0, 0), (0, 4, 1, 1, 1),
    (3, 5), (4, 5, 13, 29), (0, 3, 0, 4, 0), (3, 3), (4, 3, 11, 27), (0, 3, 1, 4, 1), (0, 4, 1, 1, 0),
    (0, 4, 1, 0, 1), (4, 18, 22, 19, 16, 17, 23), (3, 4), (4, 28, 20, 21, 4, 12),
)

def wrap(v, n):
    return lax.rem(v + n, n)


def merge(a1, a2, b1, b2):
    return jnp.maximum(a1, b1), jnp.maximum(jnp.minimum(a1, b1), jnp.maximum(a2, b2))


def kernel(
    tok_hbm, slot_hbm, unit_hbm, mask_hbm, price_out, margin_out, count_out,
    tok, give, units, mask, hot, bid, slt, prow, prep, flg, val, top, t2, sec, col, rz,
    lsem, sent, xr, br, zr, zl, sr, pr, fr, tr, cr,
):
    dp, yl = lax.axis_index("dp"), lax.axis_index("mp")
    c, yh = lax.rem(dp, 2), lax.rem(dp // 2, 2)
    z, x = lax.rem(dp // 4, Z), dp // 32
    y = yh * 2 + yl
    grp = x * 2 + yh

    def dev(x_, y_, z_, c_):
        return (((x_ * Z + z_) * 2 + y_ // 2) * 2 + c_, lax.rem(y_, 2))

    def send(src, dst, ssem, rsem, to):
        pltpu.make_async_remote_copy(
            src_ref=src, dst_ref=dst, send_sem=ssem, recv_sem=rsem, device_id=to, device_id_type=MESH
        ).start()

    def whole(ref, rsem, ssem=None):
        copy = pltpu.make_async_remote_copy(
            src_ref=ref, dst_ref=ref, send_sem=rsem if ssem is None else ssem, recv_sem=rsem,
            device_id=dev(x, y, z, 1 - c), device_id_type=MESH,
        )
        if ssem is None:
            copy.wait_recv()
        else:
            copy.wait_send()

    def far(d, n):
        return min(d, n - d)

    plane = [(dx, dy) for dx in range(X) for dy in range(Y) if dx or dy]
    plane.sort(key=lambda d: -far(d[0], X) - far(d[1], Y))
    column = [(dz, dc) for dz in range(Z) for dc in range(C) if dz or dc]
    column.sort(key=lambda d: -far(d[0], Z))

    def in_plane(dx, dy):
        return dev(wrap(x + dx, X), wrap(y + dy, Y), z, c)

    def in_column(dz, dc):
        return dev(x, y, wrap(z + dz, Z), wrap(c + dc, C))

    keep = pl.ds(pl.multiple_of(yl * HALF, 16), HALF)
    away = pl.ds(pl.multiple_of((1 - yl) * HALF, 16), HALF)
    loads = [
        pltpu.make_async_copy(mask_hbm, mask, lsem.at[0]),
        pltpu.make_async_copy(slot_hbm.at[away], give, lsem.at[1]),
        pltpu.make_async_copy(slot_hbm.at[keep], slt.at[yl, c], lsem.at[2]),
        pltpu.make_async_copy(tok_hbm, tok, lsem.at[3]),
        pltpu.make_async_copy(unit_hbm, units, lsem.at[4]),
    ]
    for load in loads:
        load.start()
    barrier = pltpu.get_barrier_semaphore()
    near = [in_plane(1, 0), in_plane(-1, 0), in_plane(0, 1), in_plane(0, -1)]
    near += [in_column(1, 0), in_column(-1, 0), in_column(0, 1)]
    for to in near:
        pl.semaphore_signal(barrier, inc=1, device_id=to, device_id_type=MESH)
    lanes = lax.broadcasted_iota(jnp.int32, (1, BUSY), 1)
    sub = lax.broadcasted_iota(jnp.int32, (8, 128), 0)
    length = mask.shape[1]

    def spread(chunk):
        prep[chunk] = jnp.broadcast_to(prow[chunk], (128, 128)).T[0:HALF, :]

    loads[4].wait()
    both = units[...].astype(jnp.float32) * UNIT
    mine = jnp.where(yl == 0, both[:, 0:HALF], both[:, HALF : 2 * HALF])
    prow[c] = jnp.concatenate([mine, jnp.zeros((1, 128 - HALF), jnp.float32)], axis=1)

    def compact():
        loads[0].wait()
        live = mask[...]
        before = lax.broadcasted_iota(jnp.int32, (length, length), 0) <= lax.broadcasted_iota(
            jnp.int32, (length, length), 1
        )
        live8 = jnp.broadcast_to(live.astype(jnp.float32), (8, length))
        rank = jnp.dot(
            live8.astype(jnp.bfloat16),
            before.astype(jnp.float32).astype(jnp.bfloat16),
            preferred_element_type=jnp.float32,
        )
        rank = jnp.where(live8 > 0, rank, 0.0)[0:1, :]
        places = lax.broadcasted_iota(jnp.int32, (BUSY, length), 0).astype(jnp.float32) + 1.0
        hot[...] = jnp.where(places == rank, 1.0, 0.0)
        total = jnp.sum(live.astype(jnp.float32), axis=1, keepdims=True)
        flg[grp] = jnp.where(lanes.astype(jnp.float32) < total, 1.0, 0.0)
        loads[3].wait()
        picked = jnp.dot(hot[...].astype(jnp.bfloat16), tok[...], preferred_element_type=jnp.float32)
        for k in range(WIDTH // 128):
            bid[yl, 0, yh, k * 128 : k * 128 + 128] = picked[:, k * 128 : k * 128 + 128].T.astype(jnp.bfloat16)

    loads[1].wait()
    loads[2].wait()
    pl.semaphore_wait(barrier, len(near))
    halves = (yl, 1 - yl)

    def rows_of(t, off, core, p=None):
        chunk = (halves[t], (off % Z) * 2 + core)
        return slt.at[chunk] if p is None else slt.at[chunk + (pl.ds(PIECES[p][0], PIECES[p][1]),)]

    def piece(dx, dy, part, p):
        ya = wrap(y + dy, Y)
        return bid.at[lax.rem(ya, 2), dx % X, ya // 2, pl.ds(part * 256 + p * 128, 128)]

    def b_at(part, j, k):
        along_x = (part == 0) == (j == 0)
        off = 0 if j == 0 else OFFS[j - 1]
        dx, dy = (off, 0) if part == 0 else (0, off)
        return dx + (k if along_x else 0), dy + (0 if along_x else k), along_x

    def b_sem(part, j, p, kind):
        if j == 0:
            return br.at[part, p * 3 + kind]
        last = 3 if part == 1 and kind == 2 else 2
        return br.at[part, 2 + j * 4 + (p if kind == p else last)]

    def b_send(part, j, p, kind):
        k = (1, -1, 1 if p == 0 else -1)[kind]
        dx, dy, along_x = b_at(part, j, -k if kind == 2 else 0)
        to = in_plane(k, 0) if along_x else in_plane(0, k)
        dst = piece(dx - k if along_x else dx, dy, part, p)
        send(piece(dx, dy, part, p), dst, sent.at[0], b_sem(part, j, p, kind), to)

    def b_take(part, j, p, kind):
        dx, dy, _ = b_at(part, j, (-1, 1, 2)[kind])
        whole(piece(dx, dy, part, p), b_sem(part, j, p, kind))

    def b_rest(part, j, far_):
        whole(bid.at[0, 0, 0, 0 : 512 if part == 0 else 256], br.at[part, 4 + j * 4 + far_])

    def sibling(t, off):
        send(rows_of(t, off, c), rows_of(t, off, c), sent.at[2], sr.at[off % Z], in_column(0, 1))

    def from_sibling(off):
        whole(slt.at[0, 0:2], sr.at[off % Z])

    left = {(t, off): len(PIECES) for t in (0, 1) for off in range(Z)}

    def landed(t, off, n=1):
        left[t, off % Z] -= n
        if left[t, off % Z] == 0:
            sibling(t, off)

    def reach(t, kind, way):
        return 4 if kind ^ t ^ way == 0 else 3

    def z_sem(t, p, way, k):
        last = k == reach(t, PIECES[p][2], way) - 1
        return zl.at[t, way, PIECES[p][2]] if last else zr.at[t, p, way, k]

    def z_send(t, p, way, k):
        step = 1 if way == 0 else -1
        src, dst = -step * k, -step * (k + 1)
        send(rows_of(t, src, c, p), rows_of(t, dst, c, p), sent.at[1], z_sem(t, p, way, k), in_column(step, 0))

    def pair(off):
        return prow.at[pl.ds((off % Z) * 2, 2)]

    def price_send(way, k):
        step = 1 if way == 0 else -1
        send(pair(-step * k), pair(-step * (k + 1)), sent.at[3], pr.at[way * 4 + k], in_column(step, 0))

    def price_take(way, k):
        off = -(k + 1) if way == 0 else k + 1
        whole(pair(off), pr.at[way * 4 + k])
        if k < (3, 2)[way]:
            price_send(way, k + 1)
        spread((off % Z) * 2)
        spread((off % Z) * 2 + 1)

    def z_take(t, p, way, k):
        off = -(k + 1) if way == 0 else k + 1
        whole(rows_of(t, off, c, p), z_sem(t, p, way, k))
        landed(t, off)
        if (t, p) == (0, 0):
            later.append((way, k))

    def z_rest(t, way, kind):
        mine, k = [p for p in PIECES if p[2] == kind], reach(t, kind, way) - 1
        off = -(k + 1) if way == 0 else k + 1
        whole(rows_of(t, off, c).at[0 : sum(p[1] for p in mine)], zl.at[t, way, kind])
        landed(t, off, len(mine))
        if (t, kind) == (0, PIECES[0][2]):
            later.append((way, k))

    def x_send(p):
        rows = pl.ds(PIECES[p][0], PIECES[p][1])
        send(give.at[rows], slt.at[yl, c, rows], sent.at[1], xr.at[p], dev(x, yh * 2 + 1 - yl, z, c))

    def x_take(p):
        whole(rows_of(1, 0, c, p), xr.at[p])
        landed(1, 0)

    seen = set()

    def values(n, off):
        acc = None
        for h in range(2):
            part = jnp.dot(
                slt[h, off * 2 : off * 2 + 2].reshape(2 * HALF, WIDTH),
                jnp.concatenate([bid[h, n, 0], bid[h, n, 1]], axis=1),
                preferred_element_type=jnp.float32,
            )
            acc = part if acc is None else acc + part
        price = prep[off * 2 : off * 2 + 2].reshape(2 * HALF, 128)
        v = acc - jnp.concatenate([price, price], axis=1)
        val[n, off * 2 : off * 2 + 2] = v.reshape(2, HALF, 256)
        if n in seen:
            m1, m2, first = top[n, 0], top[n, 1], 0
        else:
            m1, m2, first = v[0:8, :], jnp.full((8, 256), -jnp.inf, jnp.float32), 1
            seen.add(n)
        for r in range(first, 2 * HALF // 8):
            row = v[r * 8 : r * 8 + 8, :]
            m2 = jnp.maximum(m2, jnp.minimum(m1, row))
            m1 = jnp.maximum(m1, row)
        top[n, 0] = m1
        top[n, 1] = m2

    takes, sends = (b_take, z_take, x_take, b_rest, z_rest), (b_send, z_send, x_send)
    flag_at = max(i for i, op in enumerate(PLAN) if op[:2] in ((0, 0), (0, 3)))
    price_at = min(i for i, op in enumerate(PLAN) if op[0] == 0) - 1
    later = []
    for i, op in enumerate(PLAN):
        if op[0] != 1:
            while later and op[0] != 0:
                price_take(*later.pop(0))
        if op[0] == 2:
            send(prow.at[c], prow.at[c], sent.at[3], pr.at[7], in_column(0, 1))
            sibling(0, 0)
            compact()
        elif op[0] == 3:
            from_sibling(op[1])
        elif op[0] == 4:
            for unit in op[1:]:
                values(unit // 8, unit % 8)
        else:
            (takes, sends)[op[0]][op[1]](*op[2:])
        if len(later) > 1 and op[0] == 1 and PLAN[i + 1][0] != 1:
            price_take(*later.pop(0))
        if i == price_at:
            whole(prow.at[1 - c], pr.at[7])
            for way in (0, 1):
                price_send(way, 0)
            spread(0)
            spread(1)
        if i == flag_at:
            for dx in range(X):
                for dh in range(2):
                    if dx or dh:
                        send(flg.at[grp], flg.at[grp], sent.at[4], fr, in_plane(dx, 2 * dh))
    firsts, seconds = [], []
    for n in range(4):
        m1, m2 = top[n, 0], top[n, 1]
        for shift in (4, 2, 1):
            m1, m2 = merge(m1, m2, pltpu.roll(m1, shift, 0), pltpu.roll(m2, shift, 0))
        firsts += [m1[:, 0:128], m1[:, 128:256]]
        seconds += [m2[:, 0:128], m2[:, 128:256]]

    def group(dx, yh_):
        return wrap(x + dx, X) * 2 + yh_

    f, s2 = firsts[0], seconds[0]
    for i in range(GROUPS):
        f = jnp.where(sub == group(i // 2, i % 2), firsts[i], f)
        s2 = jnp.where(sub == group(i // 2, i % 2), seconds[i], s2)
    q = x * 4 + y
    t2[q, 0] = f
    t2[q, 1] = s2
    for dx, dy in plane:
        send(t2.at[q], t2.at[q], sent.at[5], tr, in_plane(dx, dy))
    whole(flg.at[0 : GROUPS - 1], fr)
    bidders = flg[0]
    for g in range(1, GROUPS):
        bidders = bidders + flg[g]
    bidders = jnp.sum(bidders, axis=1, keepdims=True)
    whole(t2.at[0:15], tr)
    f, s2 = t2[0, 0], t2[0, 1]
    for i in range(1, 16):
        f, s2 = merge(f, s2, t2[i, 0], t2[i, 1])
    sec[...] = s2
    bars = []
    for i in range(GROUPS):
        g = group(i // 2, i % 2)
        bars.append(jnp.broadcast_to(jnp.where(flg[g] > 0, sec[pl.ds(g, 1), :], jnp.inf), (HALF, 128)))
    for s in range(OWNERS):
        most_ = jnp.full((HALF, 128), -jnp.inf, jnp.float32)
        for i in range(GROUPS):
            most_ = jnp.maximum(most_, val[i // 2, s, :, (i % 2) * 128 : (i % 2) * 128 + 128] - bars[i])
        row = jnp.max(most_.T, axis=0, keepdims=True)
        row = jnp.concatenate([row, jnp.zeros((1, 128 - HALF), jnp.float32)], axis=1)
        col[s] = jnp.where(lanes == 127, bidders, row)
    for dz, dc in column:
        send(
            col.at[dz * 2 + wrap(c + dc, C)], rz.at[((Z - dz) % Z) * 2 + c], sent.at[6], cr, in_column(dz, dc)
        )
    rz[c] = col[c]
    for i, ref in enumerate((val.at[0:3, 0:8], val.at[0, 0:15], val.at[0], rz.at[0:15], flg.at[0:7], t2.at[0:15])):
        whole(ref, sent.at[i], sent.at[i])
    gap = jnp.where(flg[grp] > 0, jnp.max(jnp.where(sub == grp, f - s2, -jnp.inf), axis=0, keepdims=True), 0.0)
    margin_out[...] = jnp.dot(
        jnp.broadcast_to(gap, (8, 128)), hot[...], precision=lax.Precision.HIGHEST, preferred_element_type=jnp.float32
    )[0:1, :]
    whole(rz.at[0:15], sent.at[6], sent.at[6])
    whole(rz.at[0:15], cr)
    best, count = rz[0], rz[0]
    for i in range(1, OWNERS):
        best = jnp.maximum(best, rz[i])
        count = count + rz[i]
    price_out[...] = (prow[c] + jnp.maximum(best, 0.0))[:, 0:HALF]
    count_out[...] = count[:, 127:128].astype(jnp.int32)


def leave(*refs):
    copies = [pltpu.make_async_copy(refs[i], refs[3 + i], refs[6].at[i]) for i in range(3)]
    for copy in copies:
        copy.start()
    for copy in copies:
        copy.wait()


def on_device(tokens, slot_embed, price_units, unassigned):
    length = unassigned.shape[0]
    dma, hbm = pltpu.SemaphoreType.DMA, pl.BlockSpec(memory_space=pltpu.HBM)
    vmem = pl.BlockSpec(memory_space=pltpu.VMEM)
    f32, bf16 = jnp.float32, jnp.bfloat16
    new_prices, margins, count = pl.pallas_call(
        kernel,
        out_shape=(
            jax.ShapeDtypeStruct((1, HALF), f32),
            jax.ShapeDtypeStruct((1, length), f32),
            jax.ShapeDtypeStruct((1, 1), jnp.int32),
        ),
        in_specs=[hbm] * 4,
        out_specs=(vmem, vmem, vmem),
        scratch_shapes=[
            pltpu.VMEM((length, WIDTH), bf16),
            pltpu.VMEM((HALF, WIDTH), bf16),
            pltpu.VMEM((1, length), jnp.int32),
            pltpu.VMEM((1, length), jnp.int32),
            pltpu.VMEM((BUSY, length), f32),
            pltpu.VMEM((2, X, 2, WIDTH, BUSY), bf16),
            pltpu.VMEM((2, OWNERS, HALF, WIDTH), bf16),
            pltpu.VMEM((OWNERS, 1, 128), f32),
            pltpu.VMEM((OWNERS, HALF, 128), f32),
            pltpu.VMEM((GROUPS, 1, 128), f32),
            pltpu.VMEM((4, OWNERS, HALF, 256), f32),
            pltpu.VMEM((4, 2, 8, 256), f32),
            pltpu.VMEM((16, 2, 8, 128), f32),
            pltpu.VMEM((8, 128), f32),
            pltpu.VMEM((OWNERS, 1, 128), f32),
            pltpu.VMEM((OWNERS, 1, 128), f32),
            dma((5,)),
            dma((7,)),
            dma((len(PIECES),)),
            dma((2, 22)),
            dma((2, len(PIECES), 2, 3)),
            dma((2, 2, 2)),
            dma((Z,)),
            dma((8,)),
            dma, dma, dma,
        ],
        compiler_params=pltpu.CompilerParams(collective_id=0, has_side_effects=True, vmem_limit_bytes=32 << 20),
    )(
        *(
            pltpu.with_memory_space_constraint(v, pltpu.HBM)
            for v in (tokens, slot_embed, price_units.reshape(1, length), unassigned.reshape(1, length))
        )
    )
    new_prices, margins, count = pl.pallas_call(
        leave,
        out_shape=tuple(jax.ShapeDtypeStruct(v.shape, v.dtype) for v in (new_prices, margins, count)),
        in_specs=[vmem] * 3,
        out_specs=(hbm,) * 3,
        scratch_shapes=[dma((3,))],
        compiler_params=pltpu.CompilerParams(vmem_limit_bytes=1 << 20),
    )(new_prices, margins, count)
    return new_prices.reshape(HALF), margins.reshape(length), count.reshape(())


def solution(mesh):
    return jax.shard_map(
        on_device,
        mesh=mesh,
        in_specs=(P("dp", "mp"), P("dp", "mp"), P("dp"), P("dp")),
        out_specs=(P(("dp", "mp")), P("dp"), P()),
        check_vma=False,
    )
```
